128 devices in a mesh: lat: 16 (over y_hi, x, core), lon: 8 (over z, y_lo).
Axes of the slice: x: 4, y: 4 (y_hi: 2, y_lo: 2; y = y_hi * 2 + y_lo), z: 4, core: 2. Of those that a mesh axis runs over, the one named last changes fastest.
Arguments:
- ocean_state: bfloat16 [144, 2048, 128], P('lat', 'lon'), may hold values from -6 to 6
- cotangent: bfloat16 [144, 2048, 128], P('lat', 'lon'), may hold values from -6 to 6
- atm_embed: bfloat16 [65536, 256], P(('lat', 'lon')), may hold values from -6 to 6
- projection: bfloat16 [256, 128], replicated, may hold values from -0.375 to 0.375
- dw_kernel: float32 [7, 7, 128], replicated, may hold values from -0.875 to 0.875
- norm_gain: float32 [128], replicated, may hold values from 0.25 to 1.75
- w_in: bfloat16 [128, 512], replicated, may hold values from -0.5 to 0.5
- w_out: bfloat16 [512, 128], replicated, may hold values from -0.25 to 0.25
- margin_index: int32 [4, 144, 2048], P(None, 'lat', 'lon'), may hold values from 0 to 1023
- margin_weight: float32 [4, 144, 2048], P(None, 'lat', 'lon'), may hold values from 0.05 to 0.6
- sea_mask: int32 [144, 2048], P('lat', 'lon'), may hold values 0 or 1
Outputs:
- grad_state: float32 [144, 2048, 128], P('lat', 'lon')
- grad_embed: float32 [65536, 256], P(('lat', 'lon'))
- grad_projection: float32 [256, 128], replicated
- grad_kernel: float32 [7, 7, 128], replicated
- grad_gain: float32 [128], replicated
- grad_w_in: float32 [128, 512], replicated
- grad_w_out: float32 [512, 128], replicated
The draws below stay inside these ranges and needn't reach their ends.
All inputs are finite; a program needn't handle non-finite values. No bound on the sum of `sea_mask` on one device may be relied on, other than what follows from the above.
Results may differ from the reference program's by a relative error of at most 0.0058.
Values may be sent and summed in bfloat16 or wider, within the bound.
A program may use at most 64 MiB of HBM per device.

```python
import math
import jax
import jax.numpy as jnp
from jax import lax

LAT_DEV = 9
LON_DEV = 256
C = 128
FF = 512
E = 256
A_DEV = 512
TAPS = 7
MARGINS = 4
NLAT = 144
NLON = 2048
A_CELLS = 65536
N_LAT = 16
N_LON = 8


def with_ends(values, own_key, least, high):
    extent = values.shape
    spot = [jax.random.randint(jax.random.fold_in(own_key, axis), (), 0, extent[axis]) for axis in range(len(extent))]
    values = values.at[tuple(spot)].set(least)
    longest = extent.index(max(extent))
    spot[longest] = (spot[longest] + 1) % extent[longest]
    return values.at[tuple(spot)].set(high)


def block_scale(rng, shape, shards, least, high):
    def one(axis_at, parts):
        heights = jax.random.uniform(jax.random.fold_in(jax.random.fold_in(rng, 6), axis_at), (parts,), jnp.float32, least / len(shards), high / len(shards))
        return jnp.repeat(jnp.exp(heights), shape[axis_at] // parts).reshape((-1,) + (1,) * (len(shape) - axis_at - 1))

    level = one(*shards[0])
    for cut in shards[1:]:
        level = level * one(*cut)
    return level


def scatter_about(key, dims, scale, reach, cuts=(), kind=jnp.bfloat16):
    array = jax.random.normal(key, dims, jnp.float32) * scale
    if len(cuts) > 0:
        array = block_scale(key, dims, cuts, -0.22, 0.18) * array
    return jnp.clip(array, min=-reach, max=reach).astype(kind)


def setup_inputs(seed: int = 0) -> dict:
    seeds = jax.random.split(jax.random.key(seed), 12)
    ocean_state = scatter_about(seeds[0], (NLAT, NLON, C), 1.0, 6.0, ((0, 16), (1, 8)))
    cotangent = scatter_about(seeds[1], (NLAT, NLON, C), 1.0, 6.0, ((0, 16), (1, 8)))
    atm_embed = scatter_about(seeds[2], (A_CELLS, E), 1.0, 6.0, ((0, 128),))
    projection = scatter_about(seeds[3], (E, C), E ** -0.5, 0.375)
    dw_kernel = scatter_about(seeds[4], (TAPS, TAPS, C), (TAPS * TAPS) ** -0.5, 0.875, (), jnp.float32)
    norm_gain = jnp.clip(1.0 + 0.15 * jax.random.normal(seeds[5], (C,), jnp.float32), 0.25, 1.75)
    w_in = scatter_about(seeds[6], (C, FF), C ** -0.5, 0.5)
    w_out = scatter_about(seeds[7], (FF, C), FF ** -0.5, 0.25)
    margin_index = with_ends(jax.random.randint(seeds[8], (MARGINS, NLAT, NLON), 0, 2 * A_DEV), jax.random.fold_in(seeds[8], 1), 0, (2 * A_DEV) - 1).astype(jnp.int32)
    margin_weight = jnp.clip(jnp.exp(math.log(0.6) - 2.4849067 * jax.random.uniform(seeds[9], (MARGINS, NLAT, NLON), jnp.float32) ** block_scale(seeds[9], (MARGINS, NLAT, NLON), ((1, 16), (2, 8)), -0.2, 0.2)), 0.05, 0.6)
    sea_mask = with_ends((jax.random.randint(seeds[10], (NLAT, NLON), 0, 4) < 3).astype(jnp.int32), jax.random.fold_in(seeds[10], 1), 0, 1)
    return dict(ocean_state=ocean_state, cotangent=cotangent, atm_embed=atm_embed, projection=projection, dw_kernel=dw_kernel, norm_gain=norm_gain, w_in=w_in, w_out=w_out, margin_index=margin_index, margin_weight=margin_weight, sea_mask=sea_mask)


EPSILON = 1e-05

def wrap_pad(field):
    rows = jnp.pad(field, ((3, 3), (0, 0), (0, 0)))
    return jnp.concatenate([rows[:, -3:], rows, rows[:, :3]], axis=1)

def depthwise(padded, kernel):
    height = padded.shape[0] - 6
    width = padded.shape[1] - 6
    total = jnp.zeros((height, width, padded.shape[2]), jnp.float32)
    for row_tap in range(7):
        for col_tap in range(7):
            total = total + padded[row_tap:row_tap + height, col_tap:col_tap + width] * kernel[row_tap, col_tap]
    return total

def depthwise_back(padded, kernel):
    height = padded.shape[0] - 6
    width = padded.shape[1] - 6
    total = jnp.zeros((height, width, padded.shape[2]), jnp.float32)
    for row_tap in range(7):
        for col_tap in range(7):
            total = total + padded[6 - row_tap:6 - row_tap + height, 6 - col_tap:6 - col_tap + width] * kernel[row_tap, col_tap]
    return total

def kernel_grad(grad, padded):
    height = grad.shape[0]
    width = grad.shape[1]
    pieces = []
    for row_tap in range(7):
        for col_tap in range(7):
            pieces.append(lax.optimization_barrier(jnp.sum(grad * padded[row_tap:row_tap + height, col_tap:col_tap + width], axis=(0, 1))))
    return jnp.stack(pieces).reshape(7, 7, grad.shape[2])

def norm_forward(field):
    center = field - lax.optimization_barrier(jnp.mean(field, axis=-1, keepdims=True))
    sigma = jnp.sqrt(lax.optimization_barrier(jnp.mean(center * center, axis=-1, keepdims=True)) + EPSILON)
    return (center / sigma, sigma)

def norm_back(g_ln, normed, sigma, gain):
    gain_grad = lax.optimization_barrier(jnp.sum(g_ln * normed, axis=(0, 1)))
    g_norm = g_ln * gain
    g_field = (g_norm - lax.optimization_barrier(jnp.mean(g_norm, axis=-1, keepdims=True)) - normed * lax.optimization_barrier(jnp.mean(g_norm * normed, axis=-1, keepdims=True))) / sigma
    return (g_field, gain_grad)

def gelu_tanh(value):
    return jax.nn.gelu(value, approximate=True)

def mlp_back(ln_rows, gy_rows, w_in, w_out):
    pre_act = jnp.dot(ln_rows, w_in, preferred_element_type=jnp.float32)
    hidden, pullback = jax.vjp(gelu_tanh, pre_act)
    hidden = hidden.astype(jnp.bfloat16)
    grad_out = lax.dot_general(hidden, gy_rows, (((0,), (0,)), ((), ())), preferred_element_type=jnp.float32)
    g_hidden = lax.dot_general(gy_rows, w_out, (((1,), (1,)), ((), ())), preferred_element_type=jnp.float32)
    g_pre = pullback(g_hidden)[0].astype(jnp.bfloat16)
    grad_in = lax.dot_general(ln_rows, g_pre, (((0,), (0,)), ((), ())), preferred_element_type=jnp.float32)
    g_ln = lax.dot_general(g_pre, w_in, (((1,), (1,)), ((), ())), preferred_element_type=jnp.float32)
    return (g_ln, grad_in, grad_out)

def global_index(margin_index):
    band = (jnp.arange(NLAT, dtype=jnp.int32) // LAT_DEV)[:, None]
    tile = (jnp.arange(NLON, dtype=jnp.int32) // LON_DEV)[None, :]
    own = (band * N_LON + tile) * A_DEV + margin_index
    following = ((band + 1) * N_LON + tile) * A_DEV + margin_index - A_DEV
    chosen = jnp.where(margin_index < A_DEV, own, following)
    valid = (margin_index < A_DEV) | (band + 1 < N_LAT)
    return jnp.where(valid, chosen, A_CELLS).astype(jnp.int32)

def reference(ocean_state, cotangent, atm_embed, projection, dw_kernel, norm_gain, w_in, w_out, margin_index, margin_weight, sea_mask):
    channels = projection.shape[1]
    targets = global_index(margin_index)
    projected = jnp.dot(atm_embed, projection, preferred_element_type=jnp.float32).astype(jnp.bfloat16)
    projected = lax.optimization_barrier(projected).astype(jnp.float32)
    table = jnp.concatenate([projected, jnp.zeros((1, channels), jnp.float32)], axis=0)
    forcing = jnp.zeros((NLAT, NLON, channels), jnp.float32)
    for slot in range(MARGINS):
        forcing = forcing + margin_weight[slot][..., None] * table[targets[slot]]
    field = ocean_state.astype(jnp.float32) + forcing
    padded = wrap_pad(field)
    conv_out = depthwise(padded, dw_kernel)
    normed, sigma = norm_forward(conv_out)
    ln_cells = (normed * norm_gain).astype(jnp.bfloat16)
    g_out = cotangent.astype(jnp.float32)
    gy_cells = (sea_mask.astype(jnp.float32)[..., None] * g_out).astype(jnp.bfloat16)
    blocks = N_LAT * N_LON
    size_block = LAT_DEV * LON_DEV

    def one_block(pair):
        return mlp_back(pair[0], pair[1], w_in, w_out)
    g_ln, grad_in, grad_out = lax.map(one_block, (ln_cells.reshape(blocks, size_block, channels), gy_cells.reshape(blocks, size_block, channels)))
    g_ln = g_ln.reshape(NLAT, NLON, channels)
    g_conv, grad_gain = norm_back(g_ln, normed, sigma, norm_gain)
    grad_kernel = kernel_grad(g_conv, padded)
    grad_state = g_out + depthwise_back(wrap_pad(g_conv), dw_kernel)
    g_table = jnp.zeros((A_CELLS + 1, channels), jnp.float32)
    for slot in range(MARGINS):
        g_table = g_table.at[targets[slot].reshape(-1)].add((margin_weight[slot][..., None] * grad_state).reshape(-1, channels))
    g_projected = g_table[:A_CELLS]
    grad_embed = jnp.dot(g_projected, projection.astype(jnp.float32).T, precision=lax.Precision.HIGHEST)
    grad_projection = jnp.dot(atm_embed.astype(jnp.float32).T, g_projected, precision=lax.Precision.HIGHEST)
    return (grad_state, grad_embed, grad_projection, grad_kernel, grad_gain, lax.optimization_barrier(jnp.sum(grad_in, axis=0)), lax.optimization_barrier(jnp.sum(grad_out, axis=0)))
```

```python
import functools
import jax
import jax.numpy as jnp
from jax import lax
from jax.experimental import pallas as pl
from jax.experimental.pallas import tpu as pltpu
from jax.sharding import PartitionSpec as P

EPSILON = 1e-05


def shifted(x, axis, by):
    size = lax.axis_size(axis)
    pairs = [(i, i + by) for i in range(size) if 0 <= i + by < size]
    return lax.ppermute(x, axis, pairs)


def with_halo(block, sides, width):
    for axis, dim in sides:
        count = lax.axis_size(axis)
        forward = [(i, i + 1) for i in range(count - 1)]
        forward.append((count - 1, 0))
        backward = [(target, source) for source, target in forward]
        low = lax.ppermute(
            lax.slice_in_dim(block, block.shape[dim] - width, None, axis=dim), axis, forward
        )
        high = lax.ppermute(lax.slice_in_dim(block, 0, width, axis=dim), axis, backward)
        block = jnp.concatenate([low, block, high], axis=dim)
    return block


def depthwise(padded, kernel):
    height = padded.shape[0] - 6
    width = padded.shape[1] - 6
    total = jnp.zeros((height, width, padded.shape[2]), jnp.float32)
    for row_tap in range(7):
        for col_tap in range(7):
            total = (
                total
                + padded[row_tap : row_tap + height, col_tap : col_tap + width]
                * kernel[row_tap, col_tap]
            )
    return total


def depthwise_back(padded, kernel):
    height = padded.shape[0] - 6
    width = padded.shape[1] - 6
    total = jnp.zeros((height, width, padded.shape[2]), jnp.float32)
    for row_tap in range(7):
        for col_tap in range(7):
            total = (
                total
                + padded[6 - row_tap : 6 - row_tap + height, 6 - col_tap : 6 - col_tap + width]
                * kernel[row_tap, col_tap]
            )
    return total


def kernel_grad(grad, padded):
    height = grad.shape[0]
    width = grad.shape[1]
    pieces = []
    for row_tap in range(7):
        for col_tap in range(7):
            pieces.append(
                jnp.sum(
                    grad * padded[row_tap : row_tap + height, col_tap : col_tap + width],
                    axis=(0, 1),
                )
            )
    return jnp.stack(pieces).reshape(7, 7, grad.shape[2])


def norm_forward(field):
    center = field - jnp.mean(field, axis=-1, keepdims=True)
    sigma = jnp.sqrt(jnp.mean(center * center, axis=-1, keepdims=True) + EPSILON)
    return (center / sigma, sigma)


def norm_back(g_ln, normed, sigma, gain):
    gain_grad = jnp.sum(g_ln * normed, axis=(0, 1))
    g_norm = g_ln * gain
    g_field = (
        g_norm
        - jnp.mean(g_norm, axis=-1, keepdims=True)
        - normed * jnp.mean(g_norm * normed, axis=-1, keepdims=True)
    ) / sigma
    return (g_field, gain_grad)


def gelu_tanh(value):
    return jax.nn.gelu(value, approximate=True)


def mlp_back(ln_rows, gy_rows, w_in, w_out):
    pre_act = jnp.dot(ln_rows, w_in, preferred_element_type=jnp.float32)
    hidden, pullback = jax.vjp(gelu_tanh, pre_act)
    hidden = hidden.astype(jnp.bfloat16)
    grad_out = lax.dot_general(
        hidden, gy_rows, (((0,), (0,)), ((), ())), preferred_element_type=jnp.float32
    )
    g_hidden = lax.dot_general(
        gy_rows, w_out, (((1,), (1,)), ((), ())), preferred_element_type=jnp.float32
    )
    g_pre = pullback(g_hidden)[0].astype(jnp.bfloat16)
    grad_in = lax.dot_general(
        ln_rows, g_pre, (((0,), (0,)), ((), ())), preferred_element_type=jnp.float32
    )
    g_ln = lax.dot_general(
        g_pre, w_in, (((1,), (1,)), ((), ())), preferred_element_type=jnp.float32
    )
    return (g_ln, grad_in, grad_out)


def clear_ends(padded):
    band = lax.axis_index("lat")
    bands = lax.axis_size("lat")
    position = jnp.arange(padded.shape[0], dtype=jnp.int32)
    dropped = (band == 0) & (position < 3) | (band == bands - 1) & (position >= padded.shape[0] - 3)
    return padded * jnp.where(dropped, 0.0, 1.0).astype(jnp.float32)[:, None, None]


def margin_block(index_rows, weight_rows, slots):
    columns = jnp.arange(slots, dtype=jnp.int32)[None, :]
    dense = jnp.zeros((index_rows.shape[1], slots), jnp.float32)
    for slot in range(index_rows.shape[0]):
        dense = dense + jnp.where(
            index_rows[slot][:, None] == columns, weight_rows[slot][:, None], 0.0
        )
    return dense


def block_rows(height, width):
    limit = max(1, 2048 // width)
    best = 1
    for count in range(1, height + 1):
        if height % count == 0 and count <= limit:
            best = count
    return best


ROWS = 16
STRIDE = 55


def all_sum_kernel(
    pieces, inverse, x_ref, o_ref, send, recv, send_sem, recv_sem, out_send_sem, out_recv_sem
):
    lons = lax.axis_size("lon")
    total = lax.axis_size("lat") * lons
    me = lax.axis_index("lat") * lons + lax.axis_index("lon")
    mine = (me * inverse) % total

    def place(device):
        return {"lat": device // lons, "lon": device % lons}

    def rows_of(piece):
        return pl.ds(pl.multiple_of(piece * ROWS, ROWS), ROWS)

    barrier = pltpu.get_barrier_semaphore()

    def greet(step, carry):
        pl.semaphore_signal(
            barrier,
            inc=1,
            device_id=place((me + step) % total),
            device_id_type=pl.DeviceIdType.MESH,
        )
        return carry

    lax.fori_loop(1, total, greet, 0)
    pl.semaphore_wait(barrier, total - 1)

    def scatter(piece, carry):
        owner = (piece * STRIDE) % total

        @pl.when(owner != me)
        def _():
            slot = (me - owner + total) % total - 1
            pltpu.make_async_remote_copy(
                src_ref=x_ref.at[rows_of(piece)],
                dst_ref=recv.at[rows_of(slot)],
                send_sem=send_sem,
                recv_sem=recv_sem,
                device_id=place(owner),
                device_id_type=pl.DeviceIdType.MESH,
            ).start()

        return carry

    lax.fori_loop(0, pieces, scatter, 0)

    @pl.when(mine < pieces)
    def _():
        pltpu.make_async_copy(recv, recv, recv_sem).wait()
        own = x_ref[rows_of(mine)].astype(jnp.float32)
        others = recv[...].astype(jnp.float32).reshape(total - 1, ROWS, 128)
        send[...] = (own + jnp.sum(others, axis=0)).astype(jnp.bfloat16)
        o_ref[rows_of(mine)] = send[...]

        def gather(step, carry):
            pltpu.make_async_remote_copy(
                src_ref=send,
                dst_ref=o_ref.at[rows_of(mine)],
                send_sem=out_send_sem,
                recv_sem=out_recv_sem,
                device_id=place((me + step) % total),
                device_id_type=pl.DeviceIdType.MESH,
            ).start()
            return carry

        lax.fori_loop(1, total, gather, 0)
        part = x_ref.at[pl.ds(0, (pieces - 1) * ROWS)]
        pltpu.make_async_copy(part, part, send_sem).wait()
        out_part = o_ref.at[pl.ds(0, (pieces - 1) * ROWS)]
        pltpu.make_async_copy(out_part, out_part, out_recv_sem).wait()
        pltpu.make_async_copy(recv, recv, out_send_sem).wait()

    @pl.when(mine >= pieces)
    def _():
        pltpu.make_async_copy(x_ref, x_ref, send_sem).wait()
        pltpu.make_async_copy(o_ref, o_ref, out_recv_sem).wait()


def all_sum(partials):
    total = lax.axis_size("lat") * lax.axis_size("lon")
    shapes = [p.shape for p in partials]
    flat = jnp.concatenate([p.astype(jnp.bfloat16).reshape(-1, 128) for p in partials], axis=0)
    used = flat.shape[0]
    pieces = -(-used // ROWS)
    flat = jnp.pad(flat, ((0, pieces * ROWS - used), (0, 0)))
    summed = pl.pallas_call(
        functools.partial(all_sum_kernel, pieces, pow(STRIDE, -1, total)),
        out_shape=jax.ShapeDtypeStruct(flat.shape, flat.dtype),
        in_specs=[pl.BlockSpec(memory_space=pltpu.VMEM)],
        out_specs=pl.BlockSpec(memory_space=pltpu.VMEM),
        scratch_shapes=[
            pltpu.VMEM((ROWS, 128), jnp.bfloat16),
            pltpu.VMEM(((total - 1) * ROWS, 128), jnp.bfloat16),
        ]
        + [pltpu.SemaphoreType.DMA(())] * 4,
        compiler_params=pltpu.CompilerParams(
            collective_id=0, has_side_effects=True, vmem_limit_bytes=16 << 20
        ),
    )(flat)
    outs = []
    start = 0
    for shape in shapes:
        count = 1
        for size in shape:
            count *= size
        rows = count // 128
        outs.append(summed[start : start + rows].astype(jnp.float32).reshape(shape))
        start += rows
    return outs


def shards(
    ocean_state,
    cotangent,
    atm_embed,
    projection,
    dw_kernel,
    norm_gain,
    w_in,
    w_out,
    margin_index,
    margin_weight,
    sea_mask,
):
    cells_atm = atm_embed.shape[0]
    channels = projection.shape[1]
    height = ocean_state.shape[0]
    width = ocean_state.shape[1]
    margins = margin_index.shape[0]
    slots = 2 * cells_atm
    group = block_rows(height, width) * width
    blocks = height * width // group
    index_blocks = jnp.transpose(margin_index.reshape(margins, blocks, group), (1, 0, 2))
    weight_blocks = jnp.transpose(margin_weight.reshape(margins, blocks, group), (1, 0, 2))
    next_embed = shifted(atm_embed, "lat", -1)
    window_embed = jnp.concatenate([atm_embed, next_embed], axis=0)
    window = jnp.dot(window_embed, projection, preferred_element_type=jnp.float32).astype(
        jnp.bfloat16
    )
    window = lax.optimization_barrier(window).astype(jnp.float32)

    def forward_block(pair):
        dense = margin_block(pair[0], pair[1], slots)
        return jnp.dot(dense, window, precision=lax.Precision.HIGHEST)

    forcing = lax.map(forward_block, (index_blocks, weight_blocks)).reshape(height, width, channels)
    field = ocean_state.astype(jnp.float32) + forcing
    widened = with_halo(field, (("lon", 1),), 3)
    padded = clear_ends(with_halo(widened, (("lat", 0),), 3))
    conv_out = depthwise(padded, dw_kernel)
    normed, sigma = norm_forward(conv_out)
    ln_cells = (normed * norm_gain).astype(jnp.bfloat16)
    g_out = cotangent.astype(jnp.float32)
    gy_cells = (sea_mask.astype(jnp.float32)[..., None] * g_out).astype(jnp.bfloat16)
    g_ln, grad_in, grad_out = mlp_back(
        ln_cells.reshape(-1, channels), gy_cells.reshape(-1, channels), w_in, w_out
    )
    g_conv, grad_gain = norm_back(g_ln.reshape(height, width, channels), normed, sigma, norm_gain)
    grad_kernel = kernel_grad(g_conv, padded)
    g_widened = with_halo(g_conv.astype(jnp.bfloat16), (("lon", 1),), 3).astype(g_conv.dtype)
    g_padded = clear_ends(
        with_halo(g_widened.astype(jnp.bfloat16), (("lat", 0),), 3).astype(g_widened.dtype)
    )
    grad_state = g_out + depthwise_back(g_padded, dw_kernel)
    state_blocks = grad_state.reshape(blocks, group, channels)

    def backward_block(total, triple):
        dense = margin_block(triple[0], triple[1], slots)
        added = lax.dot_general(
            dense,
            triple[2],
            (((0,), (0,)), ((), ())),
            precision=lax.Precision.HIGHEST,
            preferred_element_type=jnp.float32,
        )
        return (total + added, None)

    g_window, unused = lax.scan(
        backward_block,
        jnp.zeros((slots, channels), jnp.float32),
        (index_blocks, weight_blocks, state_blocks),
    )
    g_window_embed = jnp.dot(
        g_window, projection.astype(jnp.float32).T, precision=lax.Precision.HIGHEST
    )
    returned = shifted(g_window_embed[cells_atm:].astype(jnp.bfloat16), "lat", 1).astype(
        jnp.float32
    )
    grad_embed = g_window_embed[:cells_atm] + returned
    grad_projection = jnp.dot(
        window_embed.astype(jnp.float32).T, g_window, precision=lax.Precision.HIGHEST
    )
    partials = (grad_projection, grad_kernel, grad_gain, grad_in, grad_out)
    totals = all_sum(partials)
    return (grad_state, grad_embed, totals[0], totals[1], totals[2], totals[3], totals[4])


def solution(mesh):
    return jax.shard_map(
        shards,
        mesh=mesh,
        in_specs=(
            P("lat", "lon", None),
            P("lat", "lon", None),
            P(("lat", "lon"), None),
            P(),
            P(),
            P(),
            P(),
            P(),
            P(None, "lat", "lon"),
            P(None, "lat", "lon"),
            P("lat", "lon"),
        ),
        out_specs=(P("lat", "lon", None), P(("lat", "lon"), None), P(), P(), P(), P(), P()),
        check_vma=False,
    )
```

```python
import functools
import jax
import jax.numpy as jnp
from jax import lax
from jax.experimental import pallas as pl
from jax.experimental.pallas import tpu as pltpu
from jax.sharding import PartitionSpec as P

EPSILON = 1e-05
ROWS = 16
STRIDE = 55
EDGE = 8
TAPS = 7
HALF = 3
MESH = pl.DeviceIdType.MESH
VMEM = pltpu.VMEM
LIMIT = 28 << 20


def here():
    lat = lax.axis_index("lat")
    lon = lax.axis_index("lon")
    lats = lax.axis_size("lat")
    lons = lax.axis_size("lon")
    return lat, lon, lats, lons


def halo_copies(pad, top_out, bottom_out, top_in, bottom_in, send_sem, recv_sem):
    lat, lon, lats, lons = here()
    height = pad.shape[0] - 2 * HALF
    width = pad.shape[1] - 2 * EDGE
    left = (lon + lons - 1) % lons
    right = (lon + 1) % lons
    has_up = lat > 0
    has_down = lat < lats - 1
    body = pl.ds(HALF, height)
    first = pl.ds(HALF, HALF)
    last = pl.ds(height, HALF)
    above = pl.ds(0, HALF)
    below = pl.ds(HALF + height, HALF)
    west = pl.ds(EDGE, EDGE)
    east = pl.ds(width, EDGE)
    west_rim = pl.ds(0, EDGE)
    east_rim = pl.ds(EDGE + width, EDGE)
    plan = [
        (top_out, bottom_in, lat - 1, lon, has_up, has_down),
        (bottom_out, top_in, lat + 1, lon, has_down, has_up),
        (pad.at[body, west], pad.at[body, east_rim], lat, left, None, None),
        (pad.at[body, east], pad.at[body, west_rim], lat, right, None, None),
        (pad.at[first, west], pad.at[below, east_rim], lat - 1, left, has_up, has_down),
        (pad.at[first, east], pad.at[below, west_rim], lat - 1, right, has_up, has_down),
        (pad.at[last, west], pad.at[above, east_rim], lat + 1, left, has_down, has_up),
        (pad.at[last, east], pad.at[above, west_rim], lat + 1, right, has_down, has_up),
    ]
    made = []
    for number, (source, target, to_lat, to_lon, sends, receives) in enumerate(plan):
        copy = pltpu.make_async_remote_copy(
            src_ref=source,
            dst_ref=target,
            send_sem=send_sem.at[number],
            recv_sem=recv_sem.at[number],
            device_id={"lat": to_lat, "lon": to_lon},
            device_id_type=MESH,
        )
        made.append((copy, sends, receives))
    return made


def guarded(condition, action):
    if condition is None:
        action()
    else:
        pl.when(condition)(action)


def halo_start(pad, top_out, bottom_out, top_in, bottom_in, send_sem, recv_sem):
    height = pad.shape[0] - 2 * HALF
    width = pad.shape[1] - 2 * EDGE
    inner = pl.ds(EDGE, width)
    top_out[...] = pad[pl.ds(HALF, HALF), inner].astype(jnp.bfloat16)
    bottom_out[...] = pad[pl.ds(height, HALF), inner].astype(jnp.bfloat16)
    copies = halo_copies(pad, top_out, bottom_out, top_in, bottom_in, send_sem, recv_sem)
    for copy, sends, _ in copies:
        guarded(sends, copy.start)


def halo_finish(pad, top_out, bottom_out, top_in, bottom_in, send_sem, recv_sem):
    lat, _, lats, _ = here()
    height = pad.shape[0] - 2 * HALF
    width = pad.shape[1] - 2 * EDGE
    inner = pl.ds(EDGE, width)
    copies = halo_copies(pad, top_out, bottom_out, top_in, bottom_in, send_sem, recv_sem)
    for copy, sends, receives in copies:
        guarded(sends, copy.wait_send)
        guarded(receives, copy.wait_recv)
    blank = jnp.zeros((HALF, pad.shape[1], pad.shape[2]), jnp.float32)

    @pl.when(lat == 0)
    def _():
        pad[pl.ds(0, HALF)] = blank

    @pl.when(lat > 0)
    def _():
        pad[pl.ds(0, HALF), inner] = top_in[...].astype(jnp.float32)

    @pl.when(lat == lats - 1)
    def _():
        pad[pl.ds(HALF + height, HALF)] = blank

    @pl.when(lat < lats - 1)
    def _():
        pad[pl.ds(HALF + height, HALF), inner] = bottom_in[...].astype(jnp.float32)


def forward_kernel(
    embed_ref, proj_ref, index_ref, weight_ref, state_ref, pad, dense,
    own, following, top_out, bottom_out, top_in, bottom_in,
    send_sem, recv_sem, window_send, window_recv,
):
    lat, lon, lats, lons = here()
    margins, height, width = index_ref.shape
    cells = embed_ref.shape[0]
    slots = 2 * cells
    left = (lon + lons - 1) % lons
    right = (lon + 1) % lons
    barrier = pltpu.get_barrier_semaphore()

    def greet(to_lat, to_lon):
        pl.semaphore_signal(
            barrier, inc=1, device_id={"lat": to_lat, "lon": to_lon}, device_id_type=MESH
        )

    greet(lat, left)
    greet(lat, right)

    @pl.when(lat > 0)
    def _():
        for to_lon in (left, lon, right):
            greet(lat - 1, to_lon)

    @pl.when(lat < lats - 1)
    def _():
        for to_lon in (left, lon, right):
            greet(lat + 1, to_lon)

    projected = jnp.dot(embed_ref[...], proj_ref[...], preferred_element_type=jnp.float32)
    own[...] = jnp.transpose(projected).astype(jnp.bfloat16)
    ends = (lat == 0).astype(jnp.int32) + (lat == lats - 1).astype(jnp.int32)
    pl.semaphore_wait(barrier, 8 - 3 * ends)

    window = pltpu.make_async_remote_copy(
        src_ref=own, dst_ref=following, send_sem=window_send, recv_sem=window_recv,
        device_id={"lat": lat - 1, "lon": lon}, device_id_type=MESH,
    )
    pl.when(lat > 0)(window.start)

    step = 32
    base = lax.broadcasted_iota(jnp.int32, (step, width), 0)

    def build(row, carry):
        picks = [index_ref[q, pl.ds(row, 1), :] for q in range(margins)]
        loads = [weight_ref[q, pl.ds(row, 1), :] for q in range(margins)]
        at = pl.ds(pl.multiple_of(row * width, 128), width)
        for start in range(0, slots, step):
            here_slots = base + start
            total = None
            for pick, load in zip(picks, loads):
                term = jnp.where(here_slots == pick, load, 0.0)
                total = term if total is None else total + term
            dense[pl.ds(start, step), at] = total.astype(jnp.bfloat16)
        return carry

    lax.fori_loop(0, height, build, 0)

    @pl.when(lat < lats - 1)
    def _():
        window.wait_recv()

    @pl.when(lat == lats - 1)
    def _():
        following[...] = jnp.zeros(following.shape, jnp.bfloat16)

    pl.when(lat > 0)(window.wait_send)

    def force(row, carry):
        at = pl.ds(pl.multiple_of(row * width, 128), width)
        forcing = jnp.dot(own[...], dense[pl.ds(0, cells), at], preferred_element_type=jnp.float32)
        forcing = forcing + jnp.dot(
            following[...], dense[pl.ds(cells, cells), at], preferred_element_type=jnp.float32
        )
        pad[row + HALF, pl.ds(EDGE, width)] = (
            state_ref[row].astype(jnp.float32) + jnp.transpose(forcing)
        )
        return carry

    lax.fori_loop(0, height, force, 0)
    rims = (pad, top_out, bottom_out, top_in, bottom_in, send_sem, recv_sem)
    halo_start(*rims)
    halo_finish(*rims)


def forward(embed, projection, index, weight, state):
    height, width, channels = state.shape
    slots = 2 * embed.shape[0]
    rim = VMEM((HALF, width, channels), jnp.bfloat16)
    return pl.pallas_call(
        forward_kernel,
        out_shape=(
            jax.ShapeDtypeStruct((height + 2 * HALF, width + 2 * EDGE, channels), jnp.float32),
            jax.ShapeDtypeStruct((slots, height * width), jnp.bfloat16),
        ),
        in_specs=[pl.BlockSpec(memory_space=VMEM)] * 5,
        out_specs=(pl.BlockSpec(memory_space=VMEM),) * 2,
        scratch_shapes=[
            VMEM((channels, embed.shape[0]), jnp.bfloat16),
            VMEM((channels, embed.shape[0]), jnp.bfloat16),
            rim, rim, rim, rim,
            pltpu.SemaphoreType.DMA((8,)),
            pltpu.SemaphoreType.DMA((8,)),
            pltpu.SemaphoreType.DMA(()),
            pltpu.SemaphoreType.DMA(()),
        ],
        compiler_params=pltpu.CompilerParams(
            collective_id=0, has_side_effects=True, vmem_limit_bytes=LIMIT
        ),
    )(embed, projection, index, weight, state)


def depthwise(pad, wide_kernel, out, height, width, flipped):
    def block(column, carry):
        start = pl.multiple_of(column * EDGE, EDGE)
        near = pad.at[:, pl.ds(start, 3 * EDGE), :]
        sums = [None] * height
        for b in range(TAPS):
            offset = EDGE - HALF + b
            rows = [near[r, offset : offset + EDGE, :] for r in range(height + 2 * HALF)]
            for a in range(TAPS):
                tap = (TAPS - 1 - a) * TAPS + TAPS - 1 - b if flipped else a * TAPS + b
                factor = wide_kernel[tap]
                for r in range(height):
                    term = rows[r + a] * factor
                    sums[r] = term if sums[r] is None else sums[r] + term
        for r in range(height):
            out[r, pl.ds(start, EDGE), :] = sums[r]
        return carry

    lax.fori_loop(0, width // EDGE, block, 0)


def kernel_grad(grad_pad, pad, small, height, width):
    channels = pad.shape[2]
    for b in range(TAPS):
        offset = EDGE - HALF + b

        def block(column, sums):
            start = pl.multiple_of(column * EDGE, EDGE)
            near = pad.at[:, pl.ds(start, 3 * EDGE), :]
            rows = [near[r, offset : offset + EDGE, :] for r in range(height + 2 * HALF)]
            grads = [
                grad_pad[r + HALF, pl.ds(pl.multiple_of(start + EDGE, EDGE), EDGE), :]
                for r in range(height)
            ]
            sums = list(sums)
            for a in range(TAPS):
                for r in range(height):
                    sums[a] = sums[a] + grads[r] * rows[r + a]
            return tuple(sums)

        zero = jnp.zeros((EDGE, channels), jnp.float32)
        sums = lax.fori_loop(0, width // EDGE, block, (zero,) * TAPS)
        for a in range(TAPS):
            small[pl.ds(a * TAPS + b, 1), :] = jnp.sum(sums[a], axis=0, keepdims=True)


def owner_of(piece, shift, total):
    return (piece * STRIDE + shift) % total


class Summing:
    def __init__(self, shift, inverse, source, result, send, recv, sems):
        self.lat, self.lon, self.lats, self.lons = here()
        self.total = self.lats * self.lons
        self.me = self.lat * self.lons + self.lon
        self.shift = shift
        self.pieces = source.shape[0] // ROWS
        self.mine = ((self.me + self.total - shift) * inverse) % self.total
        self.source, self.result, self.send, self.recv = source, result, send, recv
        self.sems = [sems.at[k] for k in range(4)]

    def place(self, device):
        return {"lat": device // self.lons, "lon": device % self.lons}

    def rows(self, piece):
        return pl.ds(pl.multiple_of(piece * ROWS, ROWS), ROWS)

    def scatter(self):
        def one(piece, carry):
            owner = owner_of(piece, self.shift, self.total)

            @pl.when(owner != self.me)
            def _():
                slot = (self.me - owner + self.total) % self.total - 1
                pltpu.make_async_remote_copy(
                    src_ref=self.source.at[self.rows(piece)],
                    dst_ref=self.recv.at[self.rows(slot)],
                    send_sem=self.sems[0],
                    recv_sem=self.sems[1],
                    device_id=self.place(owner),
                    device_id_type=MESH,
                ).start()

            return carry

        lax.fori_loop(0, self.pieces, one, 0)

    def gather(self):
        @pl.when(self.mine < self.pieces)
        def _():
            pltpu.make_async_copy(self.recv, self.recv, self.sems[1]).wait()
            own = self.source[self.rows(self.mine)].astype(jnp.float32)
            others = self.recv[...].astype(jnp.float32).reshape(self.total - 1, ROWS, 128)
            self.send[...] = (own + jnp.sum(others, axis=0)).astype(jnp.bfloat16)
            self.result[self.rows(self.mine)] = self.send[...]

            def one(step, carry):
                pltpu.make_async_remote_copy(
                    src_ref=self.send,
                    dst_ref=self.result.at[self.rows(self.mine)],
                    send_sem=self.sems[2],
                    recv_sem=self.sems[3],
                    device_id=self.place((self.me + step) % self.total),
                    device_id_type=MESH,
                ).start()
                return carry

            lax.fori_loop(1, self.total, one, 0)

    def finish(self):
        @pl.when(self.mine < self.pieces)
        def _():
            part = self.source.at[pl.ds(0, (self.pieces - 1) * ROWS)]
            pltpu.make_async_copy(part, part, self.sems[0]).wait()
            out_part = self.result.at[pl.ds(0, (self.pieces - 1) * ROWS)]
            pltpu.make_async_copy(out_part, out_part, self.sems[3]).wait()
            pltpu.make_async_copy(self.recv, self.recv, self.sems[2]).wait()

        @pl.when(self.mine >= self.pieces)
        def _():
            pltpu.make_async_copy(self.source, self.source, self.sems[0]).wait()
            pltpu.make_async_copy(self.result, self.result, self.sems[3]).wait()


def backward_kernel(
    inverse,
    pad, dense, cotangent, mask, kernel_ref, gain_ref, w_in, w_in_t, w_out_t, embed, proj_t,
    state_out, embed_out, early_out, late_out,
    wide_kernel, conv, grad_pad, state_low, g_window, grad_in, grad_out, small, gain_sum,
    back_out, back_in, top_out, bottom_out, top_in, bottom_in,
    early_send, early_one, early_recv, late_send, late_one, late_recv,
    halo_send, halo_recv, back_send, back_recv, early_sems, late_sems,
):
    lat, lon, lats, lons = here()
    total = lats * lons
    me = lat * lons + lon
    height, width, channels = cotangent.shape
    hidden = w_in.shape[1]
    cells = embed.shape[0]
    barrier = pltpu.get_barrier_semaphore()

    def greet(step, carry):
        device = (me + step) % total
        pl.semaphore_signal(
            barrier, inc=1, device_id={"lat": device // lons, "lon": device % lons},
            device_id_type=MESH,
        )
        return carry

    lax.fori_loop(1, total, greet, 0)
    for tap in range(TAPS * TAPS):
        wide_kernel[tap] = jnp.broadcast_to(kernel_ref[tap : tap + 1, :], (EDGE, channels))
    depthwise(pad, wide_kernel, conv, height, width, False)
    grad_in[...] = jnp.zeros(grad_in.shape, jnp.float32)
    grad_out[...] = jnp.zeros(grad_out.shape, jnp.float32)
    gain_sum[...] = jnp.zeros(gain_sum.shape, jnp.float32)
    gain = gain_ref[...]
    piece = 256
    c0 = 0.7978845608028654
    c1 = c0 * 0.044715

    def row_step(row, carry):
        field = conv[row]
        center = field - jnp.mean(field, axis=-1, keepdims=True)
        variance = jnp.mean(center * center, axis=-1, keepdims=True)
        inv = lax.rsqrt(variance + EPSILON)
        normed = center * inv
        ln = (normed * gain).astype(jnp.bfloat16)
        sea = jnp.transpose(
            jnp.broadcast_to(mask[pl.ds(row, 1), :].astype(jnp.float32), (channels, width))
        )
        g_y = (cotangent[row].astype(jnp.float32) * sea).astype(jnp.bfloat16)
        g_ln = None
        for start in range(0, hidden, piece):
            part = slice(start, start + piece)
            pre = jnp.dot(ln, w_in[:, part], preferred_element_type=jnp.float32)
            g_hid = jnp.dot(g_y, w_out_t[:, part], preferred_element_type=jnp.float32)
            square = pre * pre
            half = 0.5 + 0.5 * jnp.tanh(pre * (c0 + c1 * square))
            hid = (pre * half).astype(jnp.bfloat16)
            slope = half + pre * (2.0 * half * (1.0 - half)) * (c0 + (3.0 * c1) * square)
            g_pre = (g_hid * slope).astype(jnp.bfloat16)
            grad_in[:, part] += lax.dot_general(
                ln, g_pre, (((0,), (0,)), ((), ())), preferred_element_type=jnp.float32
            )
            grad_out[:, part] += lax.dot_general(
                g_y, hid, (((0,), (0,)), ((), ())), preferred_element_type=jnp.float32
            )
            term = jnp.dot(g_pre, w_in_t[part, :], preferred_element_type=jnp.float32)
            g_ln = term if g_ln is None else g_ln + term
        both = g_ln * normed
        gain_sum[...] += jnp.sum(both.reshape(width // EDGE, EDGE, channels), axis=0)
        g_n = g_ln * gain
        g_conv = (
            g_n
            - jnp.mean(g_n, axis=-1, keepdims=True)
            - normed * jnp.mean(both * gain, axis=-1, keepdims=True)
        ) * inv
        grad_pad[row + HALF, pl.ds(EDGE, width)] = g_conv
        return carry

    lax.fori_loop(0, height, row_step, 0)
    pl.semaphore_wait(barrier, total - 1)
    rims = (grad_pad, top_out, bottom_out, top_in, bottom_in, halo_send, halo_recv)
    halo_start(*rims)

    small[...] = jnp.zeros(small.shape, jnp.float32)
    kernel_grad(grad_pad, pad, small, height, width)
    small[pl.ds(TAPS * TAPS, 1), :] = jnp.sum(gain_sum[...], axis=0, keepdims=True)
    blocks = hidden // channels
    for k in range(blocks):
        columns = slice(k * channels, (k + 1) * channels)
        early_send[pl.ds(k * channels, channels)] = grad_in[:, columns].astype(jnp.bfloat16)
        early_send[pl.ds((blocks + k) * channels, channels)] = grad_out[:, columns].astype(
            jnp.bfloat16
        )
    early_send[pl.ds(2 * blocks * channels, small.shape[0])] = small[...].astype(jnp.bfloat16)
    early = Summing(0, inverse, early_send, early_out, early_one, early_recv, early_sems)
    early.scatter()
    halo_finish(*rims)

    depthwise(grad_pad, wide_kernel, conv, height, width, True)

    def state_step(row, carry):
        state = conv[row] + cotangent[row].astype(jnp.float32)
        state_out[row] = state
        state_low[pl.ds(pl.multiple_of(row * width, 128), width)] = state.astype(jnp.bfloat16)
        return carry

    lax.fori_loop(0, height, state_step, 0)
    early.gather()
    chunk = 256

    def window_step(index, carry):
        at = pl.ds(pl.multiple_of(index * chunk, chunk), chunk)
        g_window[at] = jnp.dot(dense[at, :], state_low[...], preferred_element_type=jnp.float32)
        return carry

    lax.fori_loop(cells // chunk, 2 * cells // chunk, window_step, 0)
    back_out[...] = g_window[pl.ds(cells, cells)].astype(jnp.bfloat16)
    back = pltpu.make_async_remote_copy(
        src_ref=back_out, dst_ref=back_in, send_sem=back_send, recv_sem=back_recv,
        device_id={"lat": lat + 1, "lon": lon}, device_id_type=MESH,
    )
    pl.when(lat < lats - 1)(back.start)
    lax.fori_loop(0, cells // chunk, window_step, 0)

    @pl.when(lat > 0)
    def _():
        back.wait_recv()
        g_window[pl.ds(0, cells)] += back_in[...].astype(jnp.float32)

    pl.when(lat < lats - 1)(back.wait_send)
    g_own = g_window[pl.ds(0, cells)].astype(jnp.bfloat16)
    late_send[...] = lax.dot_general(
        embed[...], g_own, (((0,), (0,)), ((), ())), preferred_element_type=jnp.float32
    ).astype(jnp.bfloat16)
    late = Summing(1, inverse, late_send, late_out, late_one, late_recv, late_sems)
    late.scatter()
    embed_out[...] = jnp.dot(g_own, proj_t[...], preferred_element_type=jnp.float32)
    late.gather()
    early.finish()
    late.finish()


def backward(pad, dense, cotangent, mask, kernel, gain, w_in, w_out, embed, projection):
    height, width, channels = cotangent.shape
    hidden = w_in.shape[1]
    cells, features = embed.shape
    total = lax.axis_size("lat") * lax.axis_size("lon")
    small_rows = -(-(TAPS * TAPS + 1) // ROWS) * ROWS
    early_rows = 2 * hidden * channels // 128 + small_rows
    late_rows = features * channels // 128
    low = jnp.bfloat16
    full = jnp.float32
    rim = VMEM((HALF, width, channels), low)
    dma = pltpu.SemaphoreType.DMA
    return pl.pallas_call(
        functools.partial(backward_kernel, pow(STRIDE, -1, total)),
        out_shape=(
            jax.ShapeDtypeStruct((height, width, channels), full),
            jax.ShapeDtypeStruct((cells, features), full),
            jax.ShapeDtypeStruct((early_rows, 128), low),
            jax.ShapeDtypeStruct((late_rows, 128), low),
        ),
        in_specs=[pl.BlockSpec(memory_space=VMEM)] * 11,
        out_specs=(pl.BlockSpec(memory_space=VMEM),) * 4,
        scratch_shapes=[
            VMEM((TAPS * TAPS, EDGE, channels), full),
            VMEM((height, width, channels), full),
            VMEM((height + 2 * HALF, width + 2 * EDGE, channels), full),
            VMEM((height * width, channels), low),
            VMEM((2 * cells, channels), full),
            VMEM((channels, hidden), full),
            VMEM((channels, hidden), full),
            VMEM((small_rows, channels), full),
            VMEM((EDGE, channels), full),
            VMEM((cells, channels), low),
            VMEM((cells, channels), low),
            rim, rim, rim, rim,
            VMEM((early_rows, 128), low),
            VMEM((ROWS, 128), low),
            VMEM(((total - 1) * ROWS, 128), low),
            VMEM((late_rows, 128), low),
            VMEM((ROWS, 128), low),
            VMEM(((total - 1) * ROWS, 128), low),
            dma((8,)), dma((8,)), dma(()), dma(()), dma((4,)), dma((4,)),
        ],
        compiler_params=pltpu.CompilerParams(
            collective_id=1, has_side_effects=True, vmem_limit_bytes=LIMIT
        ),
    )(
        pad, dense, cotangent, mask, kernel.reshape(TAPS * TAPS, channels),
        gain.reshape(1, channels), w_in, w_in.T, w_out.T, embed, projection.T,
    )


def unpack_kernel(early, late, grad_projection, grad_kernel, grad_gain, grad_in, grad_out):
    channels, hidden = grad_in.shape
    blocks = hidden // channels
    grad_projection[...] = late[...].astype(jnp.float32)
    for k in range(blocks):
        columns = slice(k * channels, (k + 1) * channels)
        grad_in[:, columns] = early[pl.ds(k * channels, channels)].astype(jnp.float32)
        grad_out[columns, :] = jnp.transpose(
            early[pl.ds((blocks + k) * channels, channels)].astype(jnp.float32)
        )
    first = 2 * blocks * channels
    small = early[pl.ds(first, early.shape[0] - first)].astype(jnp.float32)
    for a in range(TAPS):
        grad_kernel[a] = small[a * TAPS : (a + 1) * TAPS]
    grad_gain[...] = small[TAPS * TAPS : TAPS * TAPS + 1]


def unpack(early, late, channels, hidden, features):
    shapes = (
        (features, channels), (TAPS, TAPS, channels), (1, channels),
        (channels, hidden), (hidden, channels),
    )
    return pl.pallas_call(
        unpack_kernel,
        out_shape=tuple(jax.ShapeDtypeStruct(shape, jnp.float32) for shape in shapes),
        in_specs=[pl.BlockSpec(memory_space=VMEM)] * 2,
        out_specs=(pl.BlockSpec(memory_space=VMEM),) * 5,
        compiler_params=pltpu.CompilerParams(vmem_limit_bytes=8 << 20),
    )(early, late)


def shards(
    ocean_state,
    cotangent,
    atm_embed,
    projection,
    dw_kernel,
    norm_gain,
    w_in,
    w_out,
    margin_index,
    margin_weight,
    sea_mask,
):
    channels, hidden = w_in.shape
    pad, dense = forward(atm_embed, projection, margin_index, margin_weight, ocean_state)
    grad_state, grad_embed, early, late = backward(
        pad, dense, cotangent, sea_mask, dw_kernel, norm_gain, w_in, w_out, atm_embed, projection
    )
    grad_projection, grad_kernel, grad_gain, grad_in, grad_out = unpack(
        early, late, channels, hidden, atm_embed.shape[1]
    )
    return (
        grad_state, grad_embed, grad_projection, grad_kernel,
        grad_gain.reshape(channels), grad_in, grad_out,
    )


def solution(mesh):
    return jax.shard_map(
        shards,
        mesh=mesh,
        in_specs=(
            P("lat", "lon", None),
            P("lat", "lon", None),
            P(("lat", "lon"), None),
            P(),
            P(),
            P(),
            P(),
            P(),
            P(None, "lat", "lon"),
            P(None, "lat", "lon"),
            P("lat", "lon"),
        ),
        out_specs=(P("lat", "lon", None), P(("lat", "lon"), None), P(), P(), P(), P(), P()),
        check_vma=False,
    )
```

```python
import functools
import jax
import jax.numpy as jnp
from jax import lax
from jax.experimental import pallas as pl
from jax.experimental.pallas import tpu as pltpu
from jax.sharding import PartitionSpec as P

EPSILON = 1e-05
ROWS = 16
STRIDE = 55
EDGE = 8
TAPS = 7
HALF = 3
MESH = pl.DeviceIdType.MESH
VMEM = pltpu.VMEM
LIMIT = 60 << 20


def here():
    lat = lax.axis_index("lat")
    lon = lax.axis_index("lon")
    lats = lax.axis_size("lat")
    lons = lax.axis_size("lon")
    return lat, lon, lats, lons


def halo_copies(pad, top_out, bottom_out, top_in, bottom_in, send_sem, recv_sem):
    lat, lon, lats, lons = here()
    height = pad.shape[0] - 2 * HALF
    width = pad.shape[1] - 2 * EDGE
    left = (lon + lons - 1) % lons
    right = (lon + 1) % lons
    has_up = lat > 0
    has_down = lat < lats - 1
    body = pl.ds(HALF, height)
    first = pl.ds(HALF, HALF)
    last = pl.ds(height, HALF)
    above = pl.ds(0, HALF)
    below = pl.ds(HALF + height, HALF)
    west = pl.ds(EDGE, EDGE)
    east = pl.ds(width, EDGE)
    west_rim = pl.ds(0, EDGE)
    east_rim = pl.ds(EDGE + width, EDGE)
    plan = [
        (top_out, bottom_in, lat - 1, lon, has_up, has_down),
        (bottom_out, top_in, lat + 1, lon, has_down, has_up),
        (pad.at[body, west], pad.at[body, east_rim], lat, left, None, None),
        (pad.at[body, east], pad.at[body, west_rim], lat, right, None, None),
        (pad.at[first, west], pad.at[below, east_rim], lat - 1, left, has_up, has_down),
        (pad.at[first, east], pad.at[below, west_rim], lat - 1, right, has_up, has_down),
        (pad.at[last, west], pad.at[above, east_rim], lat + 1, left, has_down, has_up),
        (pad.at[last, east], pad.at[above, west_rim], lat + 1, right, has_down, has_up),
    ]
    made = []
    for number, (source, target, to_lat, to_lon, sends, receives) in enumerate(plan):
        copy = pltpu.make_async_remote_copy(
            src_ref=source,
            dst_ref=target,
            send_sem=send_sem.at[number],
            recv_sem=recv_sem.at[number],
            device_id={"lat": to_lat, "lon": to_lon},
            device_id_type=MESH,
        )
        made.append((copy, sends, receives))
    return made


def guarded(condition, action):
    if condition is None:
        action()
    else:
        pl.when(condition)(action)


def halo_start(pad, top_out, bottom_out, top_in, bottom_in, send_sem, recv_sem):
    height = pad.shape[0] - 2 * HALF
    width = pad.shape[1] - 2 * EDGE
    inner = pl.ds(EDGE, width)
    top_out[...] = pad[pl.ds(HALF, HALF), inner].astype(jnp.bfloat16)
    bottom_out[...] = pad[pl.ds(height, HALF), inner].astype(jnp.bfloat16)
    copies = halo_copies(pad, top_out, bottom_out, top_in, bottom_in, send_sem, recv_sem)
    for copy, sends, _ in copies:
        guarded(sends, copy.start)


def halo_finish(pad, top_out, bottom_out, top_in, bottom_in, send_sem, recv_sem):
    lat, _, lats, _ = here()
    height = pad.shape[0] - 2 * HALF
    width = pad.shape[1] - 2 * EDGE
    inner = pl.ds(EDGE, width)
    copies = halo_copies(pad, top_out, bottom_out, top_in, bottom_in, send_sem, recv_sem)
    for copy, sends, receives in copies:
        guarded(sends, copy.wait_send)
        guarded(receives, copy.wait_recv)
    blank = jnp.zeros((HALF, pad.shape[1], pad.shape[2]), jnp.float32)

    @pl.when(lat == 0)
    def _():
        pad[pl.ds(0, HALF)] = blank

    @pl.when(lat > 0)
    def _():
        pad[pl.ds(0, HALF), inner] = top_in[...].astype(jnp.float32)

    @pl.when(lat == lats - 1)
    def _():
        pad[pl.ds(HALF + height, HALF)] = blank

    @pl.when(lat < lats - 1)
    def _():
        pad[pl.ds(HALF + height, HALF), inner] = bottom_in[...].astype(jnp.float32)


def fetch(sources, targets, sems):
    copies = [
        pltpu.make_async_copy(source, target, sems.at[number])
        for number, (source, target) in enumerate(zip(sources, targets))
    ]
    for copy in copies:
        copy.start()
    return copies


def greet_all(barrier):
    lat, lon, lats, lons = here()
    columns = [lax.rem(lon + step, lons) for step in range(lons)]

    def one(step, carry):
        row = lax.rem(lat + step, lats)
        for number, column in enumerate(columns):
            def send(column=column):
                pl.semaphore_signal(
                    barrier, inc=1, device_id={"lat": row, "lon": column}, device_id_type=MESH
                )

            guarded(step > 0 if number == 0 else None, send)
        return carry

    lax.fori_loop(0, lats, one, 0)


def forward_part(
    barrier, embed_ref, index_ref, weight_ref, state_ref, proj_ref, loads, pad, dense, next_embed,
    own, following, top_out, bottom_out, top_in, bottom_in,
    send_sem, recv_sem, window_send, window_recv, embed_send, embed_recv,
):
    lat, lon, lats, lons = here()
    height, margins, width = index_ref.shape
    cells = embed_ref.shape[0]
    slots = 2 * cells
    index_load, weight_load, embed_load, proj_load, state_load = loads
    index_load.wait()
    weight_load.wait()
    step = 32
    base = lax.broadcasted_iota(jnp.int32, (step, width), 0)

    def build(row, carry):
        indices = index_ref[row]
        factors = weight_ref[row]
        picks = [indices[q : q + 1, :] for q in range(margins)]
        weights = [factors[q : q + 1, :] for q in range(margins)]
        at = pl.ds(pl.multiple_of(row * width, 128), width)
        for start in range(0, slots, step):
            here_slots = base + start
            total = None
            for pick, weight in zip(picks, weights):
                term = jnp.where(here_slots == pick, weight, 0.0)
                total = term if total is None else total + term
            dense[pl.ds(start, step), at] = total.astype(jnp.bfloat16)
        return carry

    lax.fori_loop(0, height, build, 0)

    embed_load.wait()
    proj_load.wait()
    projected = jnp.dot(embed_ref[...], proj_ref[...], preferred_element_type=jnp.float32)
    own[...] = jnp.transpose(projected).astype(jnp.bfloat16)
    pl.semaphore_wait(barrier, lats * lons - 1)
    window = pltpu.make_async_remote_copy(
        src_ref=own, dst_ref=following, send_sem=window_send, recv_sem=window_recv,
        device_id={"lat": lat - 1, "lon": lon}, device_id_type=MESH,
    )
    ahead = pltpu.make_async_remote_copy(
        src_ref=embed_ref, dst_ref=next_embed, send_sem=embed_send, recv_sem=embed_recv,
        device_id={"lat": lat - 1, "lon": lon}, device_id_type=MESH,
    )
    pl.when(lat > 0)(window.start)
    state_load.wait()

    def force_own(row, carry):
        at = pl.ds(pl.multiple_of(row * width, 128), width)
        forcing = jnp.dot(own[...], dense[pl.ds(0, cells), at], preferred_element_type=jnp.float32)
        pad[row + HALF, pl.ds(EDGE, width)] = (
            state_ref[row].astype(jnp.float32) + jnp.transpose(forcing)
        )
        return carry

    lax.fori_loop(0, height, force_own, 0)

    @pl.when(lat == lats - 1)
    def _():
        next_embed[...] = jnp.zeros(next_embed.shape, jnp.bfloat16)

    def force_next(row, carry):
        at = pl.ds(pl.multiple_of(row * width, 128), width)
        forcing = jnp.dot(
            following[...], dense[pl.ds(cells, cells), at], preferred_element_type=jnp.float32
        )
        pad[row + HALF, pl.ds(EDGE, width)] += jnp.transpose(forcing)
        return carry

    @pl.when(lat < lats - 1)
    def _():
        window.wait_recv()
        lax.fori_loop(0, height, force_next, 0)

    pl.when(lat > 0)(window.wait_send)
    rims = (pad, top_out, bottom_out, top_in, bottom_in, send_sem, recv_sem)
    halo_start(*rims)
    pl.when(lat > 0)(ahead.start)
    halo_finish(*rims)
    return ahead


def depthwise(pad, wide_kernel, out, height, width, flipped):
    def block(column, carry):
        start = pl.multiple_of(column * EDGE, EDGE)
        near = pad.at[:, pl.ds(start, 3 * EDGE), :]
        sums = [None] * height
        for b in range(TAPS):
            offset = EDGE - HALF + b
            rows = [near[r, offset : offset + EDGE, :] for r in range(height + 2 * HALF)]
            for a in range(TAPS):
                tap = (TAPS - 1 - a) * TAPS + TAPS - 1 - b if flipped else a * TAPS + b
                factor = wide_kernel[tap]
                for r in range(height):
                    term = rows[r + a] * factor
                    sums[r] = term if sums[r] is None else sums[r] + term
        for r in range(height):
            out[r, pl.ds(start, EDGE), :] = sums[r]
        return carry

    lax.fori_loop(0, width // EDGE, block, 0)


def kernel_grad(grad_pad, pad, small, height, width):
    channels = pad.shape[2]
    for b in range(TAPS):
        offset = EDGE - HALF + b

        def block(column, sums):
            start = pl.multiple_of(column * EDGE, EDGE)
            near = pad.at[:, pl.ds(start, 3 * EDGE), :]
            rows = [near[r, offset : offset + EDGE, :] for r in range(height + 2 * HALF)]
            grads = [
                grad_pad[r + HALF, pl.ds(pl.multiple_of(start + EDGE, EDGE), EDGE), :]
                for r in range(height)
            ]
            sums = list(sums)
            for a in range(TAPS):
                for r in range(height):
                    sums[a] = sums[a] + grads[r] * rows[r + a]
            return tuple(sums)

        zero = jnp.zeros((EDGE, channels), jnp.float32)
        sums = lax.fori_loop(0, width // EDGE, block, (zero,) * TAPS)
        for a in range(TAPS):
            small[pl.ds(a * TAPS + b, 1), :] = jnp.sum(sums[a], axis=0, keepdims=True)


def owner_of(piece, shift, total):
    return lax.rem(piece * STRIDE + shift, total)


class Summing:
    def __init__(self, shift, inverse, source, result, send, recv, sems):
        self.lat, self.lon, self.lats, self.lons = here()
        self.total = self.lats * self.lons
        self.me = self.lat * self.lons + self.lon
        self.shift = shift
        self.pieces = source.shape[0] // ROWS
        self.mine = lax.rem((self.me + self.total - shift) * inverse, self.total)
        self.source, self.result, self.send, self.recv = source, result, send, recv
        self.sems = [sems.at[k] for k in range(4)]

    def place(self, device):
        return {"lat": lax.div(device, self.lons), "lon": lax.rem(device, self.lons)}

    def rows(self, piece):
        return pl.ds(pl.multiple_of(piece * ROWS, ROWS), ROWS)

    def scatter(self):
        def one(piece, carry):
            owner = owner_of(piece, self.shift, self.total)

            @pl.when(owner != self.me)
            def _():
                slot = lax.rem(self.me - owner + self.total, self.total) - 1
                pltpu.make_async_remote_copy(
                    src_ref=self.source.at[self.rows(piece)],
                    dst_ref=self.recv.at[self.rows(slot)],
                    send_sem=self.sems[0],
                    recv_sem=self.sems[1],
                    device_id=self.place(owner),
                    device_id_type=MESH,
                ).start()

            return carry

        lax.fori_loop(0, self.pieces, one, 0)

    def gather(self):
        @pl.when(self.mine < self.pieces)
        def _():
            pltpu.make_async_copy(self.recv, self.recv, self.sems[1]).wait()
            own = self.source[self.rows(self.mine)].astype(jnp.float32)
            others = self.recv[...].astype(jnp.float32).reshape(self.total - 1, ROWS, 128)
            self.send[...] = (own + jnp.sum(others, axis=0)).astype(jnp.bfloat16)
            self.result[self.rows(self.mine)] = self.send[...]

            columns = [lax.rem(self.lon + step, self.lons) for step in range(self.lons)]

            def one(step, carry):
                row = lax.rem(self.lat + step, self.lats)
                for number, column in enumerate(columns):
                    copy = pltpu.make_async_remote_copy(
                        src_ref=self.send,
                        dst_ref=self.result.at[self.rows(self.mine)],
                        send_sem=self.sems[2],
                        recv_sem=self.sems[3],
                        device_id={"lat": row, "lon": column},
                        device_id_type=MESH,
                    )
                    guarded(step > 0 if number == 0 else None, copy.start)
                return carry

            lax.fori_loop(0, self.lats, one, 0)

    def finish(self):
        @pl.when(self.mine < self.pieces)
        def _():
            part = self.source.at[pl.ds(0, (self.pieces - 1) * ROWS)]
            pltpu.make_async_copy(part, part, self.sems[0]).wait()
            out_part = self.result.at[pl.ds(0, (self.pieces - 1) * ROWS)]
            pltpu.make_async_copy(out_part, out_part, self.sems[3]).wait()
            pltpu.make_async_copy(self.recv, self.recv, self.sems[2]).wait()

        @pl.when(self.mine >= self.pieces)
        def _():
            pltpu.make_async_copy(self.source, self.source, self.sems[0]).wait()
            pltpu.make_async_copy(self.result, self.result, self.sems[3]).wait()


def whole_kernel(
    inverse, shift,
    index_hbm, weight_hbm, embed_hbm, proj_hbm, state_hbm, kernel_hbm, cotangent_hbm, mask_hbm,
    gain_hbm, w_in_hbm, w_out_hbm,
    state_out, embed_out, early_out, late_out,
    index_ref, weight_ref, embed, proj, state_in, kernel_ref, cotangent, mask,
    gain_ref, w_in, w_out,
    pad, dense, next_embed, own, following, x_top_out, x_bottom_out, x_top_in, x_bottom_in,
    w_in_t, w_out_t, proj_t,
    wide_kernel, conv, grad_pad, state_low, g_window, grad_in, grad_out, small, gain_sum,
    back_out, back_in, g_embed, top_out, bottom_out, top_in, bottom_in,
    early_send, early_one, early_recv, late_send, late_one, late_recv,
    fetch_sem, x_send, x_recv, window_send, window_recv, ahead_send, ahead_recv,
    halo_send, halo_recv, back_send, back_recv, early_sems, late_sems, move_sem,
):
    lat, lon, lats, lons = here()
    height, width, channels = cotangent.shape
    hidden = w_in.shape[1]
    cells, features = embed.shape
    loads = fetch(
        (
            index_hbm, weight_hbm, embed_hbm, proj_hbm, state_hbm, kernel_hbm, cotangent_hbm,
            mask_hbm, gain_hbm, w_in_hbm, w_out_hbm,
        ),
        (
            index_ref, weight_ref, embed, proj, state_in, kernel_ref, cotangent,
            mask, gain_ref, w_in, w_out,
        ),
        fetch_sem,
    )
    barrier = pltpu.get_barrier_semaphore()
    greet_all(barrier)
    ahead = forward_part(
        barrier, embed, index_ref, weight_ref, state_in, proj, loads[:5], pad, dense, next_embed,
        own, following, x_top_out, x_bottom_out, x_top_in, x_bottom_in,
        x_send, x_recv, window_send, window_recv, ahead_send, ahead_recv,
    )
    for load in loads[5:]:
        load.wait()
    for tap in range(TAPS * TAPS):
        a, b = divmod(tap, TAPS)
        wide_kernel[tap] = jnp.broadcast_to(kernel_ref[a, b : b + 1, :], (EDGE, channels))
    for source, target in ((w_in, w_in_t), (w_out, w_out_t), (proj, proj_t)):
        target[...] = jnp.transpose(source[...].astype(jnp.float32)).astype(jnp.bfloat16)
    depthwise(pad, wide_kernel, conv, height, width, False)
    grad_in[...] = jnp.zeros(grad_in.shape, jnp.float32)
    grad_out[...] = jnp.zeros(grad_out.shape, jnp.float32)
    gain_sum[...] = jnp.zeros(gain_sum.shape, jnp.float32)
    gain = gain_ref[...]
    piece = 256
    c0 = 0.7978845608028654
    c1 = c0 * 0.044715

    def row_step(row, carry):
        field = conv[row]
        center = field - jnp.mean(field, axis=-1, keepdims=True)
        variance = jnp.mean(center * center, axis=-1, keepdims=True)
        inv = lax.rsqrt(variance + EPSILON)
        normed = center * inv
        ln = (normed * gain).astype(jnp.bfloat16)
        sea = jnp.transpose(
            jnp.broadcast_to(mask[pl.ds(row, 1), :].astype(jnp.float32), (channels, width))
        )
        g_y = (cotangent[row].astype(jnp.float32) * sea).astype(jnp.bfloat16)
        g_ln = None
        for start in range(0, hidden, piece):
            part = slice(start, start + piece)
            pre = jnp.dot(ln, w_in[:, part], preferred_element_type=jnp.float32)
            g_hid = jnp.dot(g_y, w_out_t[:, part], preferred_element_type=jnp.float32)
            square = pre * pre
            half = 0.5 + 0.5 * jnp.tanh(pre * (c0 + c1 * square))
            hid = (pre * half).astype(jnp.bfloat16)
            slope = half + pre * (2.0 * half * (1.0 - half)) * (c0 + (3.0 * c1) * square)
            g_pre = (g_hid * slope).astype(jnp.bfloat16)
            grad_in[:, part] += lax.dot_general(
                ln, g_pre, (((0,), (0,)), ((), ())), preferred_element_type=jnp.float32
            )
            grad_out[:, part] += lax.dot_general(
                g_y, hid, (((0,), (0,)), ((), ())), preferred_element_type=jnp.float32
            )
            term = jnp.dot(g_pre, w_in_t[part, :], preferred_element_type=jnp.float32)
            g_ln = term if g_ln is None else g_ln + term
        both = g_ln * normed
        gain_sum[...] += jnp.sum(both.reshape(width // EDGE, EDGE, channels), axis=0)
        g_n = g_ln * gain
        g_conv = (
            g_n
            - jnp.mean(g_n, axis=-1, keepdims=True)
            - normed * jnp.mean(both * gain, axis=-1, keepdims=True)
        ) * inv
        grad_pad[row + HALF, pl.ds(EDGE, width)] = g_conv
        return carry

    lax.fori_loop(0, height, row_step, 0)
    rims = (grad_pad, top_out, bottom_out, top_in, bottom_in, halo_send, halo_recv)
    halo_start(*rims)

    blocks = hidden // channels
    for k in range(blocks):
        columns = slice(k * channels, (k + 1) * channels)
        early_send[pl.ds(k * channels, channels)] = grad_in[:, columns].astype(jnp.bfloat16)
        early_send[pl.ds((blocks + k) * channels, channels)] = grad_out[:, columns].astype(
            jnp.bfloat16
        )
    early = Summing(0, inverse, early_send, early_out, early_one, early_recv, early_sems)
    early.scatter()
    small[...] = jnp.zeros(small.shape, jnp.float32)
    kernel_grad(grad_pad, pad, small, height, width)
    small[pl.ds(TAPS * TAPS, 1), :] = jnp.sum(gain_sum[...], axis=0, keepdims=True)
    late_send[pl.ds(features, small.shape[0])] = small[...].astype(jnp.bfloat16)
    halo_finish(*rims)

    depthwise(grad_pad, wide_kernel, conv, height, width, True)

    def state_step(row, carry):
        state = conv[row] + cotangent[row].astype(jnp.float32)
        conv[row] = state
        state_low[pl.ds(pl.multiple_of(row * width, 128), width)] = state.astype(jnp.bfloat16)
        return carry

    lax.fori_loop(0, height, state_step, 0)
    state_move = pltpu.make_async_copy(conv, state_out, move_sem.at[0])
    state_move.start()
    early.gather()
    chunk = 256

    def window_step(index, carry):
        at = pl.ds(pl.multiple_of(index * chunk, chunk), chunk)
        g_window[at] = jnp.dot(dense[at, :], state_low[...], preferred_element_type=jnp.float32)
        return carry

    lax.fori_loop(0, 2 * cells // chunk, window_step, 0)
    back_out[...] = g_window[pl.ds(cells, cells)].astype(jnp.bfloat16)
    pl.when(lat > 0)(ahead.wait_send)
    pl.when(lat < lats - 1)(ahead.wait_recv)
    late_send[pl.ds(0, features)] = (
        lax.dot_general(
            embed[...], g_window[pl.ds(0, cells)].astype(jnp.bfloat16),
            (((0,), (0,)), ((), ())), preferred_element_type=jnp.float32,
        )
        + lax.dot_general(
            next_embed[...], back_out[...],
            (((0,), (0,)), ((), ())), preferred_element_type=jnp.float32,
        )
    ).astype(jnp.bfloat16)
    late = Summing(shift, inverse, late_send, late_out, late_one, late_recv, late_sems)
    late.scatter()
    back = pltpu.make_async_remote_copy(
        src_ref=back_out, dst_ref=back_in, send_sem=back_send, recv_sem=back_recv,
        device_id={"lat": lat + 1, "lon": lon}, device_id_type=MESH,
    )
    pl.when(lat < lats - 1)(back.start)
    late.gather()

    @pl.when(lat > 0)
    def _():
        back.wait_recv()
        g_window[pl.ds(0, cells)] += back_in[...].astype(jnp.float32)

    pl.when(lat < lats - 1)(back.wait_send)
    g_own = g_window[pl.ds(0, cells)].astype(jnp.bfloat16)
    g_embed[...] = jnp.dot(g_own, proj_t[...], preferred_element_type=jnp.float32)
    embed_move = pltpu.make_async_copy(g_embed, embed_out, move_sem.at[1])
    embed_move.start()
    early.finish()
    late.finish()
    state_move.wait()
    embed_move.wait()


def whole(index, weight, embed, projection, state, kernel, cotangent, mask, gain, w_in, w_out):
    height, width, channels = cotangent.shape
    hidden = w_in.shape[1]
    cells, features = embed.shape
    total = lax.axis_size("lat") * lax.axis_size("lon")
    small_rows = -(-(TAPS * TAPS + 1) // ROWS) * ROWS
    early_rows = 2 * hidden * channels // 128
    late_rows = features * channels // 128 + small_rows
    low = jnp.bfloat16
    full = jnp.float32
    rim = VMEM((HALF, width, channels), low)
    padded = VMEM((height + 2 * HALF, width + 2 * EDGE, channels), full)
    dma = pltpu.SemaphoreType.DMA
    fetched = (
        index, weight, embed, projection, state, kernel, cotangent, mask,
        gain.reshape(1, channels), w_in, w_out,
    )
    return pl.pallas_call(
        functools.partial(
            whole_kernel, pow(STRIDE, -1, total), early_rows // ROWS * STRIDE % total
        ),
        out_shape=(
            jax.ShapeDtypeStruct((height, width, channels), full),
            jax.ShapeDtypeStruct((cells, features), full),
            jax.ShapeDtypeStruct((early_rows, 128), low),
            jax.ShapeDtypeStruct((late_rows, 128), low),
        ),
        in_specs=[pl.BlockSpec(memory_space=pltpu.HBM)] * len(fetched),
        out_specs=(pl.BlockSpec(memory_space=pltpu.HBM),) * 2
        + (pl.BlockSpec(memory_space=VMEM),) * 2,
        scratch_shapes=[VMEM(array.shape, array.dtype) for array in fetched]
        + [
            padded,
            VMEM((2 * cells, height * width), low),
            VMEM((cells, features), low),
            VMEM((channels, cells), low),
            VMEM((channels, cells), low),
            rim, rim, rim, rim,
            VMEM((hidden, channels), low),
            VMEM((channels, hidden), low),
            VMEM((channels, features), low),
            VMEM((TAPS * TAPS, EDGE, channels), full),
            VMEM((height, width, channels), full),
            padded,
            VMEM((height * width, channels), low),
            VMEM((2 * cells, channels), full),
            VMEM((channels, hidden), full),
            VMEM((channels, hidden), full),
            VMEM((small_rows, channels), full),
            VMEM((EDGE, channels), full),
            VMEM((cells, channels), low),
            VMEM((cells, channels), low),
            VMEM((cells, features), full),
            rim, rim, rim, rim,
            VMEM((early_rows, 128), low),
            VMEM((ROWS, 128), low),
            VMEM(((total - 1) * ROWS, 128), low),
            VMEM((late_rows, 128), low),
            VMEM((ROWS, 128), low),
            VMEM(((total - 1) * ROWS, 128), low),
            dma((len(fetched),)), dma((8,)), dma((8,)), dma(()), dma(()), dma(()), dma(()),
            dma((8,)), dma((8,)), dma(()), dma(()), dma((4,)), dma((4,)), dma((2,)),
        ],
        compiler_params=pltpu.CompilerParams(
            collective_id=0, has_side_effects=True, vmem_limit_bytes=LIMIT
        ),
    )(*fetched)


def unpack_kernel(
    early_hbm, late_hbm, state_hbm, embed_hbm,
    grad_projection, grad_kernel, grad_gain, grad_in, grad_out, grad_state, grad_embed,
    early, late, state, embed, load_sem, sems,
):
    loads = fetch(
        (early_hbm, late_hbm, state_hbm, embed_hbm), (early, late, state, embed), load_sem
    )
    for load in loads:
        load.wait()
    moves = fetch((state, embed), (grad_state, grad_embed), sems)
    channels, hidden = grad_in.shape
    features = grad_projection.shape[0]
    blocks = hidden // channels
    grad_projection[...] = late[pl.ds(0, features)].astype(jnp.float32)
    for k in range(blocks):
        columns = slice(k * channels, (k + 1) * channels)
        grad_in[:, columns] = early[pl.ds(k * channels, channels)].astype(jnp.float32)
        grad_out[columns, :] = jnp.transpose(
            early[pl.ds((blocks + k) * channels, channels)].astype(jnp.float32)
        )
    small = late[pl.ds(features, late.shape[0] - features)].astype(jnp.float32)
    for a in range(TAPS):
        grad_kernel[a] = small[a * TAPS : (a + 1) * TAPS]
    grad_gain[...] = small[TAPS * TAPS : TAPS * TAPS + 1]
    for move in moves:
        move.wait()


def unpack(early, late, state, embed, channels, hidden, features):
    shapes = (
        (features, channels), (TAPS, TAPS, channels), (1, channels),
        (channels, hidden), (hidden, channels), state.shape, embed.shape,
    )
    return pl.pallas_call(
        unpack_kernel,
        out_shape=tuple(jax.ShapeDtypeStruct(shape, jnp.float32) for shape in shapes),
        in_specs=[pl.BlockSpec(memory_space=pltpu.HBM)] * 4,
        out_specs=(pl.BlockSpec(memory_space=VMEM),) * 5
        + (pl.BlockSpec(memory_space=pltpu.HBM),) * 2,
        scratch_shapes=[VMEM(array.shape, array.dtype) for array in (early, late, state, embed)]
        + [pltpu.SemaphoreType.DMA((4,)), pltpu.SemaphoreType.DMA((2,))],
        compiler_params=pltpu.CompilerParams(vmem_limit_bytes=LIMIT),
    )(early, late, state, embed)


def shards(
    ocean_state,
    cotangent,
    atm_embed,
    projection,
    dw_kernel,
    norm_gain,
    w_in,
    w_out,
    margin_index,
    margin_weight,
    sea_mask,
):
    channels, hidden = w_in.shape
    state, embed, early, late = whole(
        jnp.transpose(margin_index, (1, 0, 2)), jnp.transpose(margin_weight, (1, 0, 2)),
        atm_embed, projection, ocean_state, dw_kernel, cotangent, sea_mask, norm_gain,
        w_in, w_out,
    )
    outs = unpack(early, late, state, embed, channels, hidden, atm_embed.shape[1])
    grad_projection, grad_kernel, grad_gain, grad_in, grad_out, grad_state, grad_embed = outs
    return (
        grad_state, grad_embed, grad_projection, grad_kernel,
        grad_gain.reshape(channels), grad_in, grad_out,
    )


def solution(mesh):
    return jax.shard_map(
        shards,
        mesh=mesh,
        in_specs=(
            P("lat", "lon", None),
            P("lat", "lon", None),
            P(("lat", "lon"), None),
            P(),
            P(),
            P(),
            P(),
            P(),
            P(None, "lat", "lon"),
            P(None, "lat", "lon"),
            P("lat", "lon"),
        ),
        out_specs=(P("lat", "lon", None), P(("lat", "lon"), None), P(), P(), P(), P(), P()),
        check_vma=False,
    )
```

```python
import functools
import jax
import jax.numpy as jnp
from jax import lax
from jax.experimental import pallas as pl
from jax.experimental.pallas import tpu as pltpu
from jax.sharding import PartitionSpec as P

EPSILON = 1e-05
ROWS = 16
STRIDE = 55
EDGE = 8
TAPS = 7
HALF = 3
MESH = pl.DeviceIdType.MESH
VMEM = pltpu.VMEM
LIMIT = 60 << 20


def here():
    lat = lax.axis_index("lat")
    lon = lax.axis_index("lon")
    lats = lax.axis_size("lat")
    lons = lax.axis_size("lon")
    return lat, lon, lats, lons


def halo_copies(pad, top_out, bottom_out, top_in, bottom_in, send_sem, recv_sem):
    lat, lon, lats, lons = here()
    height = pad.shape[0] - 2 * HALF
    width = pad.shape[1] - 2 * EDGE
    left = (lon + lons - 1) % lons
    right = (lon + 1) % lons
    has_up = lat > 0
    has_down = lat < lats - 1
    body = pl.ds(HALF, height)
    first = pl.ds(HALF, HALF)
    last = pl.ds(height, HALF)
    above = pl.ds(0, HALF)
    below = pl.ds(HALF + height, HALF)
    west = pl.ds(EDGE, EDGE)
    east = pl.ds(width, EDGE)
    west_rim = pl.ds(0, EDGE)
    east_rim = pl.ds(EDGE + width, EDGE)
    plan = [
        (top_out, bottom_in, lat - 1, lon, has_up, has_down),
        (bottom_out, top_in, lat + 1, lon, has_down, has_up),
        (pad.at[body, west], pad.at[body, east_rim], lat, left, None, None),
        (pad.at[body, east], pad.at[body, west_rim], lat, right, None, None),
        (pad.at[first, west], pad.at[below, east_rim], lat - 1, left, has_up, has_down),
        (pad.at[first, east], pad.at[below, west_rim], lat - 1, right, has_up, has_down),
        (pad.at[last, west], pad.at[above, east_rim], lat + 1, left, has_down, has_up),
        (pad.at[last, east], pad.at[above, west_rim], lat + 1, right, has_down, has_up),
    ]
    made = []
    for number, (source, target, to_lat, to_lon, sends, receives) in enumerate(plan):
        copy = pltpu.make_async_remote_copy(
            src_ref=source,
            dst_ref=target,
            send_sem=send_sem.at[number],
            recv_sem=recv_sem.at[number],
            device_id={"lat": to_lat, "lon": to_lon},
            device_id_type=MESH,
        )
        made.append((copy, sends, receives))
    return made


def guarded(condition, action):
    if condition is None:
        action()
    else:
        pl.when(condition)(action)


def halo_start(pad, top_out, bottom_out, top_in, bottom_in, send_sem, recv_sem):
    height = pad.shape[0] - 2 * HALF
    width = pad.shape[1] - 2 * EDGE
    inner = pl.ds(EDGE, width)
    top_out[...] = pad[pl.ds(HALF, HALF), inner].astype(jnp.bfloat16)
    bottom_out[...] = pad[pl.ds(height, HALF), inner].astype(jnp.bfloat16)
    copies = halo_copies(pad, top_out, bottom_out, top_in, bottom_in, send_sem, recv_sem)
    for copy, sends, _ in copies:
        guarded(sends, copy.start)


def halo_finish(pad, top_out, bottom_out, top_in, bottom_in, send_sem, recv_sem):
    lat, _, lats, _ = here()
    height = pad.shape[0] - 2 * HALF
    width = pad.shape[1] - 2 * EDGE
    inner = pl.ds(EDGE, width)
    copies = halo_copies(pad, top_out, bottom_out, top_in, bottom_in, send_sem, recv_sem)
    for copy, sends, receives in copies:
        guarded(sends, copy.wait_send)
        guarded(receives, copy.wait_recv)
    blank = jnp.zeros((HALF, pad.shape[1], pad.shape[2]), jnp.float32)

    @pl.when(lat == 0)
    def _():
        pad[pl.ds(0, HALF)] = blank

    @pl.when(lat > 0)
    def _():
        pad[pl.ds(0, HALF), inner] = top_in[...].astype(jnp.float32)

    @pl.when(lat == lats - 1)
    def _():
        pad[pl.ds(HALF + height, HALF)] = blank

    @pl.when(lat < lats - 1)
    def _():
        pad[pl.ds(HALF + height, HALF), inner] = bottom_in[...].astype(jnp.float32)


def fetch(sources, targets, sems):
    copies = [
        pltpu.make_async_copy(source, target, sems.at[number])
        for number, (source, target) in enumerate(zip(sources, targets))
    ]
    for copy in copies:
        copy.start()
    return copies


def greet_near(barrier):
    lat, lon, lats, lons = here()

    def send(row, column):
        pl.semaphore_signal(
            barrier, inc=1, device_id={"lat": row, "lon": column}, device_id_type=MESH
        )

    left = lax.rem(lon + lons - 1, lons)
    right = lax.rem(lon + 1, lons)

    @pl.when(lat > 0)
    def _():
        send(lat - 1, left)
        send(lat - 1, right)

    @pl.when(lat < lats - 1)
    def _():
        send(lat + 1, left)
        send(lat + 1, right)

    for step in range(1, lons):
        send(lat, lax.rem(lon + step, lons))
    for step in range(1, lats):
        send(lax.rem(lat + step, lats), lon)


def wait_near(barrier):
    lat, _, lats, lons = here()
    ends = (lat == 0).astype(jnp.int32) + (lat == lats - 1).astype(jnp.int32)
    pl.semaphore_wait(barrier, lats + lons + 2 - 2 * ends)


def greet_row(round_sem):
    lat, lon, lats, lons = here()
    for step in range(1, lons):
        pl.semaphore_signal(
            round_sem, inc=1, device_id={"lat": lat, "lon": lax.rem(lon + step, lons)},
            device_id_type=MESH,
        )


def forward_part(
    barrier, round_sem, embed_ref, index_ref, weight_ref, state_ref, proj_ref, loads,
    pad, dense, next_embed,
    own, following, held, top_out, bottom_out, top_in, bottom_in,
    send_sem, recv_sem, window_send, window_recv, embed_send, embed_recv,
):
    lat, lon, lats, lons = here()
    height, margins, width = index_ref.shape
    cells = embed_ref.shape[0]
    slots = 2 * cells
    index_load, weight_load, embed_load, proj_load, state_load = loads
    index_load.wait()
    weight_load.wait()
    step = 32
    base = lax.broadcasted_iota(jnp.int32, (step, width), 0)

    def build(row, carry):
        indices = index_ref[row]
        factors = weight_ref[row]
        picks = [indices[q : q + 1, :] for q in range(margins)]
        weights = [factors[q : q + 1, :] for q in range(margins)]
        merged = []
        for q in range(margins):
            sum_of = weights[q]
            for p in range(q):
                sum_of = sum_of + jnp.where(picks[p] == picks[q], weights[p], 0.0)
            merged.append(sum_of)
        at = pl.ds(pl.multiple_of(row * width, 128), width)
        for start in range(0, slots, step):
            here_slots = base + start
            total = jnp.zeros((step, width), jnp.float32)
            for pick, weight in zip(picks, merged):
                total = jnp.where(here_slots == pick, weight, total)
            dense[pl.ds(start, step), at] = total.astype(jnp.bfloat16)
        return carry

    lax.fori_loop(0, height, build, 0)

    embed_load.wait()
    proj_load.wait()
    projected = jnp.dot(embed_ref[...], proj_ref[...], preferred_element_type=jnp.float32)
    own[...] = jnp.transpose(projected).astype(jnp.bfloat16)
    wait_near(barrier)
    greet_row(round_sem)
    window = pltpu.make_async_remote_copy(
        src_ref=own, dst_ref=following, send_sem=window_send, recv_sem=window_recv,
        device_id={"lat": lat - 1, "lon": lon}, device_id_type=MESH,
    )
    ahead = pltpu.make_async_remote_copy(
        src_ref=embed_ref, dst_ref=next_embed, send_sem=embed_send, recv_sem=embed_recv,
        device_id={"lat": lat - 1, "lon": lon}, device_id_type=MESH,
    )
    pl.when(lat > 0)(window.start)
    state_load.wait()

    def force_own(row, carry):
        at = pl.ds(pl.multiple_of(row * width, 128), width)
        held[:, at] = jnp.dot(
            own[...], dense[pl.ds(0, cells), at], preferred_element_type=jnp.float32
        )
        return carry

    lax.fori_loop(0, height, force_own, 0)

    @pl.when(lat == lats - 1)
    def _():
        next_embed[...] = jnp.zeros(next_embed.shape, jnp.bfloat16)
        following[...] = jnp.zeros(following.shape, jnp.bfloat16)

    def force_next(row, carry):
        at = pl.ds(pl.multiple_of(row * width, 128), width)
        forcing = jnp.dot(
            following[...], dense[pl.ds(cells, cells), at], preferred_element_type=jnp.float32
        )
        pad[row + HALF, pl.ds(EDGE, width)] = state_ref[row].astype(
            jnp.float32
        ) + jnp.transpose(held[:, at] + forcing)
        return carry

    @pl.when(lat < lats - 1)
    def _():
        window.wait_recv()

    lax.fori_loop(0, height, force_next, 0)

    pl.when(lat > 0)(window.wait_send)
    rims = (pad, top_out, bottom_out, top_in, bottom_in, send_sem, recv_sem)
    halo_start(*rims)
    pl.when(lat > 0)(ahead.start)
    halo_finish(*rims)
    return ahead


def depthwise(pad, wide_kernel, out, height, columns, flipped):
    def block(column, carry):
        start = pl.multiple_of(column * EDGE, EDGE)
        near = pad.at[:, pl.ds(start, 3 * EDGE), :]
        sums = [None] * height
        for b in range(TAPS):
            offset = EDGE - HALF + b
            rows = [near[r, offset : offset + EDGE, :] for r in range(height + 2 * HALF)]
            for a in range(TAPS):
                tap = (TAPS - 1 - a) * TAPS + TAPS - 1 - b if flipped else a * TAPS + b
                factor = wide_kernel[tap]
                for r in range(height):
                    term = rows[r + a] * factor
                    sums[r] = term if sums[r] is None else sums[r] + term
        for r in range(height):
            out[r, pl.ds(start, EDGE), :] = sums[r]
        return carry

    lax.fori_loop(columns[0], columns[1], block, 0)


def kernel_grad(grad_pad, pad, small, height, width):
    channels = pad.shape[2]
    for b in range(TAPS):
        offset = EDGE - HALF + b

        def block(column, sums):
            start = pl.multiple_of(column * 2 * EDGE, EDGE)
            near = pad.at[:, pl.ds(start, 4 * EDGE), :]
            near_grad = grad_pad.at[:, pl.ds(start, 4 * EDGE), :]
            sums = list(sums)
            for extra in (0, EDGE):
                at = offset + extra
                rows = [near[r, at : at + EDGE, :] for r in range(height + 2 * HALF)]
                for r in range(height):
                    grad = near_grad[r + HALF, EDGE + extra : 2 * EDGE + extra, :]
                    for a in range(TAPS):
                        sums[a] = sums[a] + grad * rows[r + a]
            return tuple(sums)

        zero = jnp.zeros((EDGE, channels), jnp.float32)
        sums = lax.fori_loop(0, width // (2 * EDGE), block, (zero,) * TAPS)
        for a in range(TAPS):
            small[pl.ds(a * TAPS + b, 1), :] = jnp.sum(sums[a], axis=0, keepdims=True)


def owner_of(piece, shift, total):
    return lax.rem(piece * STRIDE + shift, total)


class Summing:
    def __init__(self, shift, inverse, source, result, send, recv, sems):
        self.lat, self.lon, self.lats, self.lons = here()
        self.total = self.lats * self.lons
        self.me = self.lat * self.lons + self.lon
        self.shift = shift
        self.pieces = source.shape[0] // ROWS
        self.mine = lax.rem((self.me + self.total - shift) * inverse, self.total)
        self.source, self.result, self.send, self.recv = source, result, send, recv
        self.sems = [sems.at[k] for k in range(4)]

    def place(self, device):
        return {"lat": lax.div(device, self.lons), "lon": lax.rem(device, self.lons)}

    def rows(self, piece):
        return pl.ds(pl.multiple_of(piece * ROWS, ROWS), ROWS)

    def scatter(self):
        def one(piece, carry):
            owner = owner_of(piece, self.shift, self.total)

            @pl.when(owner != self.me)
            def _():
                slot = lax.rem(self.me - owner + self.total, self.total) - 1
                pltpu.make_async_remote_copy(
                    src_ref=self.source.at[self.rows(piece)],
                    dst_ref=self.recv.at[self.rows(slot)],
                    send_sem=self.sems[0],
                    recv_sem=self.sems[1],
                    device_id=self.place(owner),
                    device_id_type=MESH,
                ).start()

            return carry

        lax.fori_loop(0, self.pieces, one, 0)

    def gather(self):
        @pl.when(self.mine < self.pieces)
        def _():
            pltpu.make_async_copy(self.recv, self.recv, self.sems[1]).wait()
            own = self.source[self.rows(self.mine)].astype(jnp.float32)
            others = self.recv[...].astype(jnp.float32).reshape(self.total - 1, ROWS, 128)
            self.send[...] = (own + jnp.sum(others, axis=0)).astype(jnp.bfloat16)
            self.result[self.rows(self.mine)] = self.send[...]

            columns = [lax.rem(self.lon + step, self.lons) for step in range(self.lons)]

            def one(step, carry):
                row = lax.rem(self.lat + step, self.lats)
                for number, column in enumerate(columns):
                    copy = pltpu.make_async_remote_copy(
                        src_ref=self.send,
                        dst_ref=self.result.at[self.rows(self.mine)],
                        send_sem=self.sems[2],
                        recv_sem=self.sems[3],
                        device_id={"lat": row, "lon": column},
                        device_id_type=MESH,
                    )
                    guarded(step > 0 if number == 0 else None, copy.start)
                return carry

            lax.fori_loop(0, self.lats, one, 0)

    def finish(self):
        @pl.when(self.mine < self.pieces)
        def _():
            part = self.source.at[pl.ds(0, (self.pieces - 1) * ROWS)]
            pltpu.make_async_copy(part, part, self.sems[0]).wait()
            out_part = self.result.at[pl.ds(0, (self.pieces - 1) * ROWS)]
            pltpu.make_async_copy(out_part, out_part, self.sems[3]).wait()
            pltpu.make_async_copy(self.recv, self.recv, self.sems[2]).wait()

        @pl.when(self.mine >= self.pieces)
        def _():
            pltpu.make_async_copy(self.source, self.source, self.sems[0]).wait()
            pltpu.make_async_copy(self.result, self.result, self.sems[3]).wait()


def whole_kernel(
    inverse, shift,
    index_hbm, weight_hbm, embed_hbm, proj_hbm, state_hbm, kernel_hbm, cotangent_hbm, mask_hbm,
    gain_hbm, w_in_hbm, w_out_hbm,
    state_out, embed_out, early_out, late_out,
    index_ref, weight_ref, embed, proj, state_in, kernel_ref, cotangent, mask,
    gain_ref, w_in, w_out,
    pad, dense, next_embed, own, following, held, x_top_out, x_bottom_out, x_top_in, x_bottom_in,
    normed_rows, inv_rows, ln_row, g_y_row, g_ln_row,
    w_in_t, w_out_t, proj_t,
    wide_kernel, conv, grad_pad, state_low, g_window, grad_in, grad_out, small, gain_sum,
    back_out, back_in, g_embed, top_out, bottom_out, top_in, bottom_in,
    early_send, early_one, early_recv, late_send, late_one, late_recv,
    fetch_sem, x_send, x_recv, window_send, window_recv, ahead_send, ahead_recv,
    halo_send, halo_recv, back_send, back_recv, early_sems, late_sems, move_sem, round_sem,
):
    lat, lon, lats, lons = here()
    height, width, channels = cotangent.shape
    hidden = w_in.shape[1]
    cells, features = embed.shape
    loads = fetch(
        (
            index_hbm, weight_hbm, embed_hbm, proj_hbm, state_hbm, kernel_hbm, cotangent_hbm,
            mask_hbm, gain_hbm, w_in_hbm, w_out_hbm,
        ),
        (
            index_ref, weight_ref, embed, proj, state_in, kernel_ref, cotangent,
            mask, gain_ref, w_in, w_out,
        ),
        fetch_sem,
    )
    barrier = pltpu.get_barrier_semaphore()
    greet_near(barrier)
    ahead = forward_part(
        barrier, round_sem, embed, index_ref, weight_ref, state_in, proj, loads[:5],
        pad, dense, next_embed,
        own, following, held, x_top_out, x_bottom_out, x_top_in, x_bottom_in,
        x_send, x_recv, window_send, window_recv, ahead_send, ahead_recv,
    )
    for load in loads[5:]:
        load.wait()
    for tap in range(TAPS * TAPS):
        a, b = divmod(tap, TAPS)
        wide_kernel[tap] = jnp.broadcast_to(kernel_ref[a, b : b + 1, :], (EDGE, channels))
    for source, target in ((w_in, w_in_t), (w_out, w_out_t), (proj, proj_t)):
        target[...] = jnp.transpose(source[...].astype(jnp.float32)).astype(jnp.bfloat16)
    blocks_wide = width // EDGE
    depthwise(pad, wide_kernel, conv, height, (0, blocks_wide), False)
    grad_in[...] = jnp.zeros(grad_in.shape, jnp.float32)
    grad_out[...] = jnp.zeros(grad_out.shape, jnp.float32)
    gain_sum[...] = jnp.zeros(gain_sum.shape, jnp.float32)
    gain = gain_ref[...]
    piece = 256
    c0 = 0.7978845608028654
    c1 = c0 * 0.044715

    def norm_of(row):
        field = conv[row]
        center = field - jnp.mean(field, axis=-1, keepdims=True)
        variance = jnp.mean(center * center, axis=-1, keepdims=True)
        inv = jnp.broadcast_to(lax.rsqrt(variance + EPSILON), field.shape)
        normed = center * inv
        sea = jnp.transpose(
            jnp.broadcast_to(mask[pl.ds(row, 1), :].astype(jnp.float32), (channels, width))
        )
        normed_rows[row] = normed
        inv_rows[row] = inv
        ln_row[...] = (normed * gain).astype(jnp.bfloat16)
        g_y_row[...] = (cotangent[row].astype(jnp.float32) * sea).astype(jnp.bfloat16)

    def mlp_of():
        ln = ln_row[...]
        g_y = g_y_row[...]
        g_ln = None
        for start in range(0, hidden, piece):
            part = slice(start, start + piece)
            pre = jnp.dot(ln, w_in[:, part], preferred_element_type=jnp.float32)
            g_hid = jnp.dot(g_y, w_out_t[:, part], preferred_element_type=jnp.float32)
            square = pre * pre
            half = 0.5 + 0.5 * jnp.tanh(pre * (c0 + c1 * square))
            hid = (pre * half).astype(jnp.bfloat16)
            slope = half + pre * (2.0 * half * (1.0 - half)) * (c0 + (3.0 * c1) * square)
            g_pre = (g_hid * slope).astype(jnp.bfloat16)
            grad_in[:, part] += lax.dot_general(
                ln, g_pre, (((0,), (0,)), ((), ())), preferred_element_type=jnp.float32
            )
            grad_out[:, part] += lax.dot_general(
                g_y, hid, (((0,), (0,)), ((), ())), preferred_element_type=jnp.float32
            )
            term = jnp.dot(g_pre, w_in_t[part, :], preferred_element_type=jnp.float32)
            g_ln = term if g_ln is None else g_ln + term
        g_ln_row[...] = g_ln

    def norm_back_of(row):
        normed = normed_rows[row]
        g_ln = g_ln_row[...]
        both = g_ln * normed
        gain_sum[...] += jnp.sum(both.reshape(width // EDGE, EDGE, channels), axis=0)
        g_n = g_ln * gain
        g_conv = (
            g_n
            - jnp.mean(g_n, axis=-1, keepdims=True)
            - normed * jnp.mean(both * gain, axis=-1, keepdims=True)
        ) * inv_rows[row]
        grad_pad[row + HALF, pl.ds(EDGE, width)] = g_conv

    def row_step(row, carry):
        norm_back_of(row - 1)
        mlp_of()
        norm_of(row + 1)
        return carry

    norm_of(0)
    mlp_of()
    norm_of(1)
    lax.fori_loop(1, height - 1, row_step, 0)
    norm_back_of(height - 2)
    mlp_of()
    norm_back_of(height - 1)
    rims = (grad_pad, top_out, bottom_out, top_in, bottom_in, halo_send, halo_recv)
    halo_start(*rims)

    blocks = hidden // channels
    for k in range(blocks):
        columns = slice(k * channels, (k + 1) * channels)
        early_send[pl.ds(k * channels, channels)] = grad_in[:, columns].astype(jnp.bfloat16)
        early_send[pl.ds((blocks + k) * channels, channels)] = grad_out[:, columns].astype(
            jnp.bfloat16
        )
    early = Summing(0, inverse, early_send, early_out, early_one, early_recv, early_sems)
    pl.semaphore_wait(round_sem, lons - 1)
    early.scatter()
    small[...] = jnp.zeros(small.shape, jnp.float32)
    kernel_grad(grad_pad, pad, small, height, width)
    small[pl.ds(TAPS * TAPS, 1), :] = jnp.sum(gain_sum[...], axis=0, keepdims=True)
    late_send[pl.ds(features, small.shape[0])] = small[...].astype(jnp.bfloat16)
    halo_finish(*rims)

    depthwise(grad_pad, wide_kernel, conv, height, (0, blocks_wide), True)

    def state_step(row, carry):
        state = conv[row] + cotangent[row].astype(jnp.float32)
        conv[row] = state
        state_low[pl.ds(pl.multiple_of(row * width, 128), width)] = state.astype(jnp.bfloat16)
        return carry

    lax.fori_loop(0, height, state_step, 0)
    state_move = pltpu.make_async_copy(conv, state_out, move_sem.at[0])
    state_move.start()
    early.gather()
    chunk = 256

    def window_step(index, carry):
        at = pl.ds(pl.multiple_of(index * chunk, chunk), chunk)
        g_window[at] = jnp.dot(dense[at, :], state_low[...], preferred_element_type=jnp.float32)
        return carry

    lax.fori_loop(0, 2 * cells // chunk, window_step, 0)
    back_out[...] = g_window[pl.ds(cells, cells)].astype(jnp.bfloat16)
    pl.when(lat > 0)(ahead.wait_send)
    pl.when(lat < lats - 1)(ahead.wait_recv)
    late_send[pl.ds(0, features)] = (
        lax.dot_general(
            embed[...], g_window[pl.ds(0, cells)].astype(jnp.bfloat16),
            (((0,), (0,)), ((), ())), preferred_element_type=jnp.float32,
        )
        + lax.dot_general(
            next_embed[...], back_out[...],
            (((0,), (0,)), ((), ())), preferred_element_type=jnp.float32,
        )
    ).astype(jnp.bfloat16)
    late = Summing(shift, inverse, late_send, late_out, late_one, late_recv, late_sems)
    late.scatter()
    back = pltpu.make_async_remote_copy(
        src_ref=back_out, dst_ref=back_in, send_sem=back_send, recv_sem=back_recv,
        device_id={"lat": lat + 1, "lon": lon}, device_id_type=MESH,
    )
    pl.when(lat < lats - 1)(back.start)
    late.gather()

    @pl.when(lat > 0)
    def _():
        back.wait_recv()
        g_window[pl.ds(0, cells)] += back_in[...].astype(jnp.float32)

    pl.when(lat < lats - 1)(back.wait_send)
    g_own = g_window[pl.ds(0, cells)].astype(jnp.bfloat16)
    g_embed[...] = jnp.dot(g_own, proj_t[...], preferred_element_type=jnp.float32)
    embed_move = pltpu.make_async_copy(g_embed, embed_out, move_sem.at[1])
    embed_move.start()
    early.finish()
    late.finish()
    state_move.wait()
    embed_move.wait()


def whole(index, weight, embed, projection, state, kernel, cotangent, mask, gain, w_in, w_out):
    height, width, channels = cotangent.shape
    hidden = w_in.shape[1]
    cells, features = embed.shape
    total = lax.axis_size("lat") * lax.axis_size("lon")
    small_rows = -(-(TAPS * TAPS + 1) // ROWS) * ROWS
    early_rows = 2 * hidden * channels // 128
    late_rows = features * channels // 128 + small_rows
    low = jnp.bfloat16
    full = jnp.float32
    rim = VMEM((HALF, width, channels), low)
    padded = VMEM((height + 2 * HALF, width + 2 * EDGE, channels), full)
    dma = pltpu.SemaphoreType.DMA
    fetched = (
        index, weight, embed, projection, state, kernel, cotangent, mask,
        gain.reshape(1, channels), w_in, w_out,
    )
    return pl.pallas_call(
        functools.partial(
            whole_kernel, pow(STRIDE, -1, total), early_rows // ROWS * STRIDE % total
        ),
        out_shape=(
            jax.ShapeDtypeStruct((height, width, channels), full),
            jax.ShapeDtypeStruct((cells, features), full),
            jax.ShapeDtypeStruct((early_rows, 128), low),
            jax.ShapeDtypeStruct((late_rows, 128), low),
        ),
        in_specs=[pl.BlockSpec(memory_space=pltpu.HBM)] * len(fetched),
        out_specs=(pl.BlockSpec(memory_space=pltpu.HBM),) * 2
        + (pl.BlockSpec(memory_space=VMEM),) * 2,
        scratch_shapes=[VMEM(array.shape, array.dtype) for array in fetched]
        + [
            padded,
            VMEM((2 * cells, height * width), low),
            VMEM((cells, features), low),
            VMEM((channels, cells), low),
            VMEM((channels, cells), low),
            VMEM((channels, height * width), full),
            rim, rim, rim, rim,
            VMEM((height, width, channels), full),
            VMEM((height, width, channels), full),
            VMEM((width, channels), low),
            VMEM((width, channels), low),
            VMEM((width, channels), full),
            VMEM((hidden, channels), low),
            VMEM((channels, hidden), low),
            VMEM((channels, features), low),
            VMEM((TAPS * TAPS, EDGE, channels), full),
            VMEM((height, width, channels), full),
            padded,
            VMEM((height * width, channels), low),
            VMEM((2 * cells, channels), full),
            VMEM((channels, hidden), full),
            VMEM((channels, hidden), full),
            VMEM((small_rows, channels), full),
            VMEM((EDGE, channels), full),
            VMEM((cells, channels), low),
            VMEM((cells, channels), low),
            VMEM((cells, features), full),
            rim, rim, rim, rim,
            VMEM((early_rows, 128), low),
            VMEM((ROWS, 128), low),
            VMEM(((total - 1) * ROWS, 128), low),
            VMEM((late_rows, 128), low),
            VMEM((ROWS, 128), low),
            VMEM(((total - 1) * ROWS, 128), low),
            dma((len(fetched),)), dma((8,)), dma((8,)), dma(()), dma(()), dma(()), dma(()),
            dma((8,)), dma((8,)), dma(()), dma(()), dma((4,)), dma((4,)), dma((2,)),
            pltpu.SemaphoreType.REGULAR,
        ],
        compiler_params=pltpu.CompilerParams(
            collective_id=0, has_side_effects=True, vmem_limit_bytes=LIMIT
        ),
    )(*fetched)


def unpack_kernel(
    early_hbm, late_hbm, state_hbm, embed_hbm,
    projection_out, kernel_out, gain_out, in_out, out_out, state_out, embed_out,
    early, late, state, embed, grad_projection, grad_kernel, grad_gain, grad_in, grad_out,
    load_sem, sems,
):
    loads = fetch(
        (early_hbm, late_hbm, state_hbm, embed_hbm), (early, late, state, embed), load_sem
    )
    channels, hidden = grad_in.shape
    features = grad_projection.shape[0]
    blocks = hidden // channels
    moves = [
        pltpu.make_async_copy(source, target, sems.at[number])
        for number, (source, target) in enumerate(
            (
                (state, state_out), (embed, embed_out), (grad_projection, projection_out),
                (grad_kernel, kernel_out), (grad_gain, gain_out), (grad_in, in_out),
                (grad_out, out_out),
            )
        )
    ]
    loads[0].wait()
    for k in range(blocks):
        columns = slice(k * channels, (k + 1) * channels)
        grad_in[:, columns] = early[pl.ds(k * channels, channels)].astype(jnp.float32)
    moves[5].start()
    loads[1].wait()
    grad_projection[...] = late[pl.ds(0, features)].astype(jnp.float32)
    moves[2].start()
    small = late[pl.ds(features, late.shape[0] - features)].astype(jnp.float32)
    for a in range(TAPS):
        grad_kernel[a] = small[a * TAPS : (a + 1) * TAPS]
    grad_gain[...] = small[TAPS * TAPS : TAPS * TAPS + 1]
    moves[3].start()
    moves[4].start()
    loads[2].wait()
    moves[0].start()
    loads[3].wait()
    moves[1].start()
    for k in range(blocks):
        columns = slice(k * channels, (k + 1) * channels)
        grad_out[columns, :] = jnp.transpose(
            early[pl.ds((blocks + k) * channels, channels)].astype(jnp.float32)
        )
    moves[6].start()
    for move in moves:
        move.wait()


def unpack(early, late, state, embed, channels, hidden, features):
    grads = (
        (features, channels), (TAPS, TAPS, channels), (1, channels),
        (channels, hidden), (hidden, channels),
    )
    shapes = grads + (state.shape, embed.shape)
    return pl.pallas_call(
        unpack_kernel,
        out_shape=tuple(jax.ShapeDtypeStruct(shape, jnp.float32) for shape in shapes),
        in_specs=[pl.BlockSpec(memory_space=pltpu.HBM)] * 4,
        out_specs=(pl.BlockSpec(memory_space=pltpu.HBM),) * 7,
        scratch_shapes=[VMEM(array.shape, array.dtype) for array in (early, late, state, embed)]
        + [VMEM(shape, jnp.float32) for shape in grads]
        + [pltpu.SemaphoreType.DMA((4,)), pltpu.SemaphoreType.DMA((7,))],
        compiler_params=pltpu.CompilerParams(vmem_limit_bytes=LIMIT),
    )(early, late, state, embed)


def shards(
    ocean_state,
    cotangent,
    atm_embed,
    projection,
    dw_kernel,
    norm_gain,
    w_in,
    w_out,
    margin_index,
    margin_weight,
    sea_mask,
):
    channels, hidden = w_in.shape
    state, embed, early, late = whole(
        jnp.transpose(margin_index, (1, 0, 2)), jnp.transpose(margin_weight, (1, 0, 2)),
        atm_embed, projection, ocean_state, dw_kernel, cotangent, sea_mask, norm_gain,
        w_in, w_out,
    )
    outs = unpack(early, late, state, embed, channels, hidden, atm_embed.shape[1])
    grad_projection, grad_kernel, grad_gain, grad_in, grad_out, grad_state, grad_embed = outs
    return (
        grad_state, grad_embed, grad_projection, grad_kernel,
        grad_gain.reshape(channels), grad_in, grad_out,
    )


def solution(mesh):
    return jax.shard_map(
        shards,
        mesh=mesh,
        in_specs=(
            P("lat", "lon", None),
            P("lat", "lon", None),
            P(("lat", "lon"), None),
            P(),
            P(),
            P(),
            P(),
            P(),
            P(None, "lat", "lon"),
            P(None, "lat", "lon"),
            P("lat", "lon"),
        ),
        out_specs=(P("lat", "lon", None), P(("lat", "lon"), None), P(), P(), P(), P(), P()),
        check_vma=False,
    )
```

```python
import functools
import jax
import jax.numpy as jnp
from jax import lax
from jax.experimental import pallas as pl
from jax.experimental.pallas import tpu as pltpu
from jax.sharding import PartitionSpec as P

EPSILON = 1e-05
ROWS = 16
STRIDE = 55
EDGE = 8
TAPS = 7
HALF = 3
MESH = pl.DeviceIdType.MESH
VMEM = pltpu.VMEM
LIMIT = 60 << 20


def here():
    lat = lax.axis_index("lat")
    lon = lax.axis_index("lon")
    lats = lax.axis_size("lat")
    lons = lax.axis_size("lon")
    return lat, lon, lats, lons


def halo_copies(pad, top_out, bottom_out, top_in, bottom_in, send_sem, recv_sem):
    lat, lon, lats, lons = here()
    height = pad.shape[0] - 2 * HALF
    width = pad.shape[1] - 2 * EDGE
    left = (lon + lons - 1) % lons
    right = (lon + 1) % lons
    has_up = lat > 0
    has_down = lat < lats - 1
    body = pl.ds(HALF, height)
    first = pl.ds(HALF, HALF)
    last = pl.ds(height, HALF)
    above = pl.ds(0, HALF)
    below = pl.ds(HALF + height, HALF)
    west = pl.ds(EDGE, EDGE)
    east = pl.ds(width, EDGE)
    west_rim = pl.ds(0, EDGE)
    east_rim = pl.ds(EDGE + width, EDGE)
    plan = [
        (top_out, bottom_in, lat - 1, lon, has_up, has_down),
        (bottom_out, top_in, lat + 1, lon, has_down, has_up),
        (pad.at[body, west], pad.at[body, east_rim], lat, left, None, None),
        (pad.at[body, east], pad.at[body, west_rim], lat, right, None, None),
        (pad.at[first, west], pad.at[below, east_rim], lat - 1, left, has_up, has_down),
        (pad.at[first, east], pad.at[below, west_rim], lat - 1, right, has_up, has_down),
        (pad.at[last, west], pad.at[above, east_rim], lat + 1, left, has_down, has_up),
        (pad.at[last, east], pad.at[above, west_rim], lat + 1, right, has_down, has_up),
    ]
    made = []
    for number, (source, target, to_lat, to_lon, sends, receives) in enumerate(plan):
        copy = pltpu.make_async_remote_copy(
            src_ref=source,
            dst_ref=target,
            send_sem=send_sem.at[number],
            recv_sem=recv_sem.at[number],
            device_id={"lat": to_lat, "lon": to_lon},
            device_id_type=MESH,
        )
        made.append((copy, sends, receives))
    return made


def guarded(condition, action):
    if condition is None:
        action()
    else:
        pl.when(condition)(action)


def halo_start(pad, top_out, bottom_out, top_in, bottom_in, send_sem, recv_sem):
    height = pad.shape[0] - 2 * HALF
    width = pad.shape[1] - 2 * EDGE
    inner = pl.ds(EDGE, width)
    top_out[...] = pad[pl.ds(HALF, HALF), inner].astype(jnp.bfloat16)
    bottom_out[...] = pad[pl.ds(height, HALF), inner].astype(jnp.bfloat16)
    copies = halo_copies(pad, top_out, bottom_out, top_in, bottom_in, send_sem, recv_sem)
    for copy, sends, _ in copies:
        guarded(sends, copy.start)


def halo_finish(pad, top_out, bottom_out, top_in, bottom_in, send_sem, recv_sem):
    lat, _, lats, _ = here()
    height = pad.shape[0] - 2 * HALF
    width = pad.shape[1] - 2 * EDGE
    inner = pl.ds(EDGE, width)
    copies = halo_copies(pad, top_out, bottom_out, top_in, bottom_in, send_sem, recv_sem)
    for copy, sends, receives in copies:
        guarded(sends, copy.wait_send)
        guarded(receives, copy.wait_recv)
    blank = jnp.zeros((HALF, pad.shape[1], pad.shape[2]), jnp.float32)

    @pl.when(lat == 0)
    def _():
        pad[pl.ds(0, HALF)] = blank

    @pl.when(lat > 0)
    def _():
        pad[pl.ds(0, HALF), inner] = top_in[...].astype(jnp.float32)

    @pl.when(lat == lats - 1)
    def _():
        pad[pl.ds(HALF + height, HALF)] = blank

    @pl.when(lat < lats - 1)
    def _():
        pad[pl.ds(HALF + height, HALF), inner] = bottom_in[...].astype(jnp.float32)


def fetch(sources, targets, sems):
    copies = [
        pltpu.make_async_copy(source, target, sems.at[number])
        for number, (source, target) in enumerate(zip(sources, targets))
    ]
    for copy in copies:
        copy.start()
    return copies


def greet_near(barrier):
    lat, lon, lats, lons = here()

    def send(row, column):
        pl.semaphore_signal(
            barrier, inc=1, device_id={"lat": row, "lon": column}, device_id_type=MESH
        )

    left = lax.rem(lon + lons - 1, lons)
    right = lax.rem(lon + 1, lons)

    @pl.when(lat > 0)
    def _():
        send(lat - 1, left)
        send(lat - 1, right)

    @pl.when(lat < lats - 1)
    def _():
        send(lat + 1, left)
        send(lat + 1, right)

    for step in range(1, lons):
        send(lat, lax.rem(lon + step, lons))
    for step in range(1, lats):
        send(lax.rem(lat + step, lats), lon)


def wait_near(barrier):
    lat, _, lats, lons = here()
    ends = (lat == 0).astype(jnp.int32) + (lat == lats - 1).astype(jnp.int32)
    pl.semaphore_wait(barrier, lats + lons + 2 - 2 * ends)


def greet_row(round_sem):
    lat, lon, lats, lons = here()
    for step in range(1, lons):
        pl.semaphore_signal(
            round_sem, inc=1, device_id={"lat": lat, "lon": lax.rem(lon + step, lons)},
            device_id_type=MESH,
        )


def forward_part(
    barrier, round_sem, embed_ref, index_ref, weight_ref, state_ref, proj_ref, loads,
    pad, dense, next_embed,
    own, following, held, top_out, bottom_out, top_in, bottom_in,
    send_sem, recv_sem, window_send, window_recv, embed_send, embed_recv,
):
    lat, lon, lats, lons = here()
    height, margins, width = index_ref.shape
    cells = embed_ref.shape[0]
    slots = 2 * cells
    index_load, weight_load, embed_load, proj_load, state_load = loads
    index_load.wait()
    weight_load.wait()
    step = 32
    base = lax.broadcasted_iota(jnp.int32, (step, width), 0)

    def build(row, carry):
        indices = index_ref[row]
        factors = weight_ref[row]
        picks = [indices[q : q + 1, :] for q in range(margins)]
        weights = [factors[q : q + 1, :] for q in range(margins)]
        merged = []
        for q in range(margins):
            sum_of = weights[q]
            for p in range(q):
                sum_of = sum_of + jnp.where(picks[p] == picks[q], weights[p], 0.0)
            merged.append(sum_of)
        at = pl.ds(pl.multiple_of(row * width, 128), width)
        for start in range(0, slots, step):
            here_slots = base + start
            total = jnp.zeros((step, width), jnp.float32)
            for pick, weight in zip(picks, merged):
                total = jnp.where(here_slots == pick, weight, total)
            dense[pl.ds(start, step), at] = total.astype(jnp.bfloat16)
        return carry

    lax.fori_loop(0, height, build, 0)

    embed_load.wait()
    proj_load.wait()
    projected = jnp.dot(embed_ref[...], proj_ref[...], preferred_element_type=jnp.float32)
    own[...] = jnp.transpose(projected).astype(jnp.bfloat16)
    wait_near(barrier)
    greet_row(round_sem)
    window = pltpu.make_async_remote_copy(
        src_ref=own, dst_ref=following, send_sem=window_send, recv_sem=window_recv,
        device_id={"lat": lat - 1, "lon": lon}, device_id_type=MESH,
    )
    ahead = pltpu.make_async_remote_copy(
        src_ref=embed_ref, dst_ref=next_embed, send_sem=embed_send, recv_sem=embed_recv,
        device_id={"lat": lat - 1, "lon": lon}, device_id_type=MESH,
    )
    pl.when(lat > 0)(window.start)
    state_load.wait()

    def force_own(row, carry):
        at = pl.ds(pl.multiple_of(row * width, 128), width)
        held[:, at] = jnp.dot(
            own[...], dense[pl.ds(0, cells), at], preferred_element_type=jnp.float32
        )
        return carry

    lax.fori_loop(0, height, force_own, 0)

    @pl.when(lat == lats - 1)
    def _():
        next_embed[...] = jnp.zeros(next_embed.shape, jnp.bfloat16)
        following[...] = jnp.zeros(following.shape, jnp.bfloat16)

    def force_next(row, carry):
        at = pl.ds(pl.multiple_of(row * width, 128), width)
        forcing = jnp.dot(
            following[...], dense[pl.ds(cells, cells), at], preferred_element_type=jnp.float32
        )
        pad[row + HALF, pl.ds(EDGE, width)] = state_ref[row].astype(
            jnp.float32
        ) + jnp.transpose(held[:, at] + forcing)
        return carry

    @pl.when(lat < lats - 1)
    def _():
        window.wait_recv()

    lax.fori_loop(0, height, force_next, 0)

    pl.when(lat > 0)(window.wait_send)
    rims = (pad, top_out, bottom_out, top_in, bottom_in, send_sem, recv_sem)
    halo_start(*rims)
    halo_finish(*rims)
    pl.when(lat > 0)(ahead.start)
    return ahead


def depthwise(pad, wide_kernel, out, height, columns, flipped):
    def block(column, carry):
        start = pl.multiple_of(column * EDGE, EDGE)
        near = pad.at[:, pl.ds(start, 3 * EDGE), :]
        sums = [None] * height
        for b in range(TAPS):
            offset = EDGE - HALF + b
            rows = [near[r, offset : offset + EDGE, :] for r in range(height + 2 * HALF)]
            for a in range(TAPS):
                tap = (TAPS - 1 - a) * TAPS + TAPS - 1 - b if flipped else a * TAPS + b
                factor = wide_kernel[tap]
                for r in range(height):
                    term = rows[r + a] * factor
                    sums[r] = term if sums[r] is None else sums[r] + term
        for r in range(height):
            out[r, pl.ds(start, EDGE), :] = sums[r]
        return carry

    lax.fori_loop(columns[0], columns[1], block, 0)


def kernel_grad(grad_pad, pad, small, height, width):
    channels = pad.shape[2]
    for b in range(TAPS):
        offset = EDGE - HALF + b

        def block(column, sums):
            start = pl.multiple_of(column * 2 * EDGE, EDGE)
            near = pad.at[:, pl.ds(start, 4 * EDGE), :]
            near_grad = grad_pad.at[:, pl.ds(start, 4 * EDGE), :]
            sums = list(sums)
            for extra in (0, EDGE):
                at = offset + extra
                rows = [near[r, at : at + EDGE, :] for r in range(height + 2 * HALF)]
                for r in range(height):
                    grad = near_grad[r + HALF, EDGE + extra : 2 * EDGE + extra, :]
                    for a in range(TAPS):
                        sums[a] = sums[a] + grad * rows[r + a]
            return tuple(sums)

        zero = jnp.zeros((EDGE, channels), jnp.float32)
        sums = lax.fori_loop(0, width // (2 * EDGE), block, (zero,) * TAPS)
        for a in range(TAPS):
            small[pl.ds(a * TAPS + b, 1), :] = jnp.sum(sums[a], axis=0, keepdims=True)


def owner_of(piece, shift, total):
    return lax.rem(piece * STRIDE + shift, total)


class Summing:
    def __init__(self, shift, inverse, source, result, send, recv, sems):
        self.lat, self.lon, self.lats, self.lons = here()
        self.total = self.lats * self.lons
        self.me = self.lat * self.lons + self.lon
        self.shift = shift
        self.pieces = source.shape[0] // ROWS
        self.mine = lax.rem((self.me + self.total - shift) * inverse, self.total)
        self.source, self.result, self.send, self.recv = source, result, send, recv
        self.sems = [sems.at[k] for k in range(4)]

    def place(self, device):
        return {"lat": lax.div(device, self.lons), "lon": lax.rem(device, self.lons)}

    def rows(self, piece):
        return pl.ds(pl.multiple_of(piece * ROWS, ROWS), ROWS)

    def scatter(self):
        def one(piece, carry):
            owner = owner_of(piece, self.shift, self.total)

            @pl.when(owner != self.me)
            def _():
                slot = lax.rem(self.me - owner + self.total, self.total) - 1
                pltpu.make_async_remote_copy(
                    src_ref=self.source.at[self.rows(piece)],
                    dst_ref=self.recv.at[self.rows(slot)],
                    send_sem=self.sems[0],
                    recv_sem=self.sems[1],
                    device_id=self.place(owner),
                    device_id_type=MESH,
                ).start()

            return carry

        lax.fori_loop(0, self.pieces, one, 0)

    def gather(self):
        @pl.when(self.mine < self.pieces)
        def _():
            pltpu.make_async_copy(self.recv, self.recv, self.sems[1]).wait()
            own = self.source[self.rows(self.mine)].astype(jnp.float32)
            others = self.recv[...].astype(jnp.float32).reshape(self.total - 1, ROWS, 128)
            self.send[...] = (own + jnp.sum(others, axis=0)).astype(jnp.bfloat16)
            self.result[self.rows(self.mine)] = self.send[...]

            columns = [lax.rem(self.lon + step, self.lons) for step in range(self.lons)]

            def one(step, carry):
                row = lax.rem(self.lat + step, self.lats)
                for number, column in enumerate(columns):
                    copy = pltpu.make_async_remote_copy(
                        src_ref=self.send,
                        dst_ref=self.result.at[self.rows(self.mine)],
                        send_sem=self.sems[2],
                        recv_sem=self.sems[3],
                        device_id={"lat": row, "lon": column},
                        device_id_type=MESH,
                    )
                    guarded(step > 0 if number == 0 else None, copy.start)
                return carry

            lax.fori_loop(0, self.lats, one, 0)

    def finish(self):
        @pl.when(self.mine < self.pieces)
        def _():
            part = self.source.at[pl.ds(0, (self.pieces - 1) * ROWS)]
            pltpu.make_async_copy(part, part, self.sems[0]).wait()
            out_part = self.result.at[pl.ds(0, (self.pieces - 1) * ROWS)]
            pltpu.make_async_copy(out_part, out_part, self.sems[3]).wait()
            pltpu.make_async_copy(self.recv, self.recv, self.sems[2]).wait()

        @pl.when(self.mine >= self.pieces)
        def _():
            pltpu.make_async_copy(self.source, self.source, self.sems[0]).wait()
            pltpu.make_async_copy(self.result, self.result, self.sems[3]).wait()


def whole_kernel(
    inverse, shift,
    index_hbm, weight_hbm, embed_hbm, proj_hbm, state_hbm, kernel_hbm, cotangent_hbm, mask_hbm,
    gain_hbm, w_in_hbm, w_out_hbm,
    state_out, embed_out, early_out, late_out,
    index_ref, weight_ref, embed, proj, state_in, kernel_ref, cotangent, mask,
    gain_ref, w_in, w_out,
    pad, dense, next_embed, own, following, held, x_top_out, x_bottom_out, x_top_in, x_bottom_in,
    normed_rows, inv_rows, ln_row, g_y_row, g_ln_row,
    w_in_t, w_out_t, proj_t,
    wide_kernel, conv, grad_pad, state_low, g_window, grad_in, grad_out, small, gain_sum,
    back_out, back_in, g_embed, top_out, bottom_out, top_in, bottom_in,
    early_send, early_one, early_recv, late_send, late_one, late_recv,
    fetch_sem, x_send, x_recv, window_send, window_recv, ahead_send, ahead_recv,
    halo_send, halo_recv, back_send, back_recv, early_sems, late_sems, move_sem, round_sem,
):
    lat, lon, lats, lons = here()
    height, width, channels = cotangent.shape
    hidden = w_in.shape[1]
    cells, features = embed.shape
    loads = fetch(
        (
            index_hbm, weight_hbm, embed_hbm, proj_hbm, state_hbm, kernel_hbm, cotangent_hbm,
            mask_hbm, gain_hbm, w_in_hbm, w_out_hbm,
        ),
        (
            index_ref, weight_ref, embed, proj, state_in, kernel_ref, cotangent,
            mask, gain_ref, w_in, w_out,
        ),
        fetch_sem,
    )
    barrier = pltpu.get_barrier_semaphore()
    greet_near(barrier)
    ahead = forward_part(
        barrier, round_sem, embed, index_ref, weight_ref, state_in, proj, loads[:5],
        pad, dense, next_embed,
        own, following, held, x_top_out, x_bottom_out, x_top_in, x_bottom_in,
        x_send, x_recv, window_send, window_recv, ahead_send, ahead_recv,
    )
    for load in loads[5:]:
        load.wait()
    for tap in range(TAPS * TAPS):
        a, b = divmod(tap, TAPS)
        wide_kernel[tap] = jnp.broadcast_to(kernel_ref[a, b : b + 1, :], (EDGE, channels))
    for source, target in ((w_in, w_in_t), (w_out, w_out_t), (proj, proj_t)):
        target[...] = jnp.transpose(source[...].astype(jnp.float32)).astype(jnp.bfloat16)
    blocks_wide = width // EDGE
    depthwise(pad, wide_kernel, conv, height, (0, blocks_wide), False)
    grad_in[...] = jnp.zeros(grad_in.shape, jnp.float32)
    grad_out[...] = jnp.zeros(grad_out.shape, jnp.float32)
    gain_sum[...] = jnp.zeros(gain_sum.shape, jnp.float32)
    gain = gain_ref[...]
    piece = 256
    c0 = 0.7978845608028654
    c1 = c0 * 0.044715

    def norm_of(row):
        field = conv[row]
        center = field - jnp.mean(field, axis=-1, keepdims=True)
        variance = jnp.mean(center * center, axis=-1, keepdims=True)
        inv = jnp.broadcast_to(lax.rsqrt(variance + EPSILON), field.shape)
        normed = center * inv
        sea = jnp.transpose(
            jnp.broadcast_to(mask[pl.ds(row, 1), :].astype(jnp.float32), (channels, width))
        )
        normed_rows[row] = normed
        inv_rows[row] = inv
        ln_row[...] = (normed * gain).astype(jnp.bfloat16)
        g_y_row[...] = (cotangent[row].astype(jnp.float32) * sea).astype(jnp.bfloat16)

    def mlp_of():
        ln = ln_row[...]
        g_y = g_y_row[...]
        g_ln = None
        for start in range(0, hidden, piece):
            part = slice(start, start + piece)
            pre = jnp.dot(ln, w_in[:, part], preferred_element_type=jnp.float32)
            g_hid = jnp.dot(g_y, w_out_t[:, part], preferred_element_type=jnp.float32)
            square = pre * pre
            half = 0.5 + 0.5 * jnp.tanh(pre * (c0 + c1 * square))
            hid = (pre * half).astype(jnp.bfloat16)
            slope = half + pre * (2.0 * half * (1.0 - half)) * (c0 + (3.0 * c1) * square)
            g_pre = (g_hid * slope).astype(jnp.bfloat16)
            grad_in[:, part] += lax.dot_general(
                ln, g_pre, (((0,), (0,)), ((), ())), preferred_element_type=jnp.float32
            )
            grad_out[:, part] += lax.dot_general(
                g_y, hid, (((0,), (0,)), ((), ())), preferred_element_type=jnp.float32
            )
            term = jnp.dot(g_pre, w_in_t[part, :], preferred_element_type=jnp.float32)
            g_ln = term if g_ln is None else g_ln + term
        g_ln_row[...] = g_ln

    def norm_back_of(row):
        normed = normed_rows[row]
        g_ln = g_ln_row[...]
        both = g_ln * normed
        gain_sum[...] += jnp.sum(both.reshape(width // EDGE, EDGE, channels), axis=0)
        g_n = g_ln * gain
        g_conv = (
            g_n
            - jnp.mean(g_n, axis=-1, keepdims=True)
            - normed * jnp.mean(both * gain, axis=-1, keepdims=True)
        ) * inv_rows[row]
        grad_pad[row + HALF, pl.ds(EDGE, width)] = g_conv

    def row_step(row, carry):
        norm_back_of(row - 1)
        mlp_of()
        norm_of(row + 1)
        return carry

    norm_of(0)
    mlp_of()
    norm_of(1)
    lax.fori_loop(1, height - 1, row_step, 0)
    norm_back_of(height - 2)
    mlp_of()
    norm_back_of(height - 1)
    rims = (grad_pad, top_out, bottom_out, top_in, bottom_in, halo_send, halo_recv)
    halo_start(*rims)

    blocks = hidden // channels
    for k in range(blocks):
        columns = slice(k * channels, (k + 1) * channels)
        early_send[pl.ds(k * channels, channels)] = grad_in[:, columns].astype(jnp.bfloat16)
        early_send[pl.ds((blocks + k) * channels, channels)] = grad_out[:, columns].astype(
            jnp.bfloat16
        )
    early = Summing(0, inverse, early_send, early_out, early_one, early_recv, early_sems)
    pl.semaphore_wait(round_sem, lons - 1)
    early.scatter()
    small[...] = jnp.zeros(small.shape, jnp.float32)
    kernel_grad(grad_pad, pad, small, height, width)
    small[pl.ds(TAPS * TAPS, 1), :] = jnp.sum(gain_sum[...], axis=0, keepdims=True)
    late_send[pl.ds(features, small.shape[0])] = small[...].astype(jnp.bfloat16)
    halo_finish(*rims)

    depthwise(grad_pad, wide_kernel, conv, height, (0, blocks_wide), True)

    def state_step(row, carry):
        state = conv[row] + cotangent[row].astype(jnp.float32)
        conv[row] = state
        state_low[pl.ds(pl.multiple_of(row * width, 128), width)] = state.astype(jnp.bfloat16)
        return carry

    lax.fori_loop(0, height, state_step, 0)
    state_move = pltpu.make_async_copy(conv, state_out, move_sem.at[0])
    state_move.start()
    chunk = 256

    def window_step(index, carry):
        at = pl.ds(pl.multiple_of(index * chunk, chunk), chunk)
        g_window[at] = jnp.dot(dense[at, :], state_low[...], preferred_element_type=jnp.float32)
        return carry

    lax.fori_loop(0, 2 * cells // chunk, window_step, 0)
    back_out[...] = g_window[pl.ds(cells, cells)].astype(jnp.bfloat16)
    pl.when(lat > 0)(ahead.wait_send)
    pl.when(lat < lats - 1)(ahead.wait_recv)
    late_send[pl.ds(0, features)] = (
        lax.dot_general(
            embed[...], g_window[pl.ds(0, cells)].astype(jnp.bfloat16),
            (((0,), (0,)), ((), ())), preferred_element_type=jnp.float32,
        )
        + lax.dot_general(
            next_embed[...], back_out[...],
            (((0,), (0,)), ((), ())), preferred_element_type=jnp.float32,
        )
    ).astype(jnp.bfloat16)
    late = Summing(shift, inverse, late_send, late_out, late_one, late_recv, late_sems)
    late.scatter()
    early.gather()
    back = pltpu.make_async_remote_copy(
        src_ref=back_out, dst_ref=back_in, send_sem=back_send, recv_sem=back_recv,
        device_id={"lat": lat + 1, "lon": lon}, device_id_type=MESH,
    )
    pl.when(lat < lats - 1)(back.start)
    late.gather()

    @pl.when(lat > 0)
    def _():
        back.wait_recv()
        g_window[pl.ds(0, cells)] += back_in[...].astype(jnp.float32)

    pl.when(lat < lats - 1)(back.wait_send)
    g_own = g_window[pl.ds(0, cells)].astype(jnp.bfloat16)
    g_embed[...] = jnp.dot(g_own, proj_t[...], preferred_element_type=jnp.float32)
    embed_move = pltpu.make_async_copy(g_embed, embed_out, move_sem.at[1])
    embed_move.start()
    early.finish()
    late.finish()
    state_move.wait()
    embed_move.wait()


def whole(index, weight, embed, projection, state, kernel, cotangent, mask, gain, w_in, w_out):
    height, width, channels = cotangent.shape
    hidden = w_in.shape[1]
    cells, features = embed.shape
    total = lax.axis_size("lat") * lax.axis_size("lon")
    small_rows = -(-(TAPS * TAPS + 1) // ROWS) * ROWS
    early_rows = 2 * hidden * channels // 128
    late_rows = features * channels // 128 + small_rows
    low = jnp.bfloat16
    full = jnp.float32
    rim = VMEM((HALF, width, channels), low)
    padded = VMEM((height + 2 * HALF, width + 2 * EDGE, channels), full)
    dma = pltpu.SemaphoreType.DMA
    fetched = (
        index, weight, embed, projection, state, kernel, cotangent, mask,
        gain.reshape(1, channels), w_in, w_out,
    )
    return pl.pallas_call(
        functools.partial(
            whole_kernel, pow(STRIDE, -1, total), early_rows // ROWS * STRIDE % total
        ),
        out_shape=(
            jax.ShapeDtypeStruct((height, width, channels), full),
            jax.ShapeDtypeStruct((cells, features), full),
            jax.ShapeDtypeStruct((early_rows, 128), low),
            jax.ShapeDtypeStruct((late_rows, 128), low),
        ),
        in_specs=[pl.BlockSpec(memory_space=pltpu.HBM)] * len(fetched),
        out_specs=(pl.BlockSpec(memory_space=pltpu.HBM),) * 2
        + (pl.BlockSpec(memory_space=VMEM),) * 2,
        scratch_shapes=[VMEM(array.shape, array.dtype) for array in fetched]
        + [
            padded,
            VMEM((2 * cells, height * width), low),
            VMEM((cells, features), low),
            VMEM((channels, cells), low),
            VMEM((channels, cells), low),
            VMEM((channels, height * width), full),
            rim, rim, rim, rim,
            VMEM((height, width, channels), full),
            VMEM((height, width, channels), full),
            VMEM((width, channels), low),
            VMEM((width, channels), low),
            VMEM((width, channels), full),
            VMEM((hidden, channels), low),
            VMEM((channels, hidden), low),
            VMEM((channels, features), low),
            VMEM((TAPS * TAPS, EDGE, channels), full),
            VMEM((height, width, channels), full),
            padded,
            VMEM((height * width, channels), low),
            VMEM((2 * cells, channels), full),
            VMEM((channels, hidden), full),
            VMEM((channels, hidden), full),
            VMEM((small_rows, channels), full),
            VMEM((EDGE, channels), full),
            VMEM((cells, channels), low),
            VMEM((cells, channels), low),
            VMEM((cells, features), full),
            rim, rim, rim, rim,
            VMEM((early_rows, 128), low),
            VMEM((ROWS, 128), low),
            VMEM(((total - 1) * ROWS, 128), low),
            VMEM((late_rows, 128), low),
            VMEM((ROWS, 128), low),
            VMEM(((total - 1) * ROWS, 128), low),
            dma((len(fetched),)), dma((8,)), dma((8,)), dma(()), dma(()), dma(()), dma(()),
            dma((8,)), dma((8,)), dma(()), dma(()), dma((4,)), dma((4,)), dma((2,)),
            pltpu.SemaphoreType.REGULAR,
        ],
        compiler_params=pltpu.CompilerParams(
            collective_id=0, has_side_effects=True, vmem_limit_bytes=LIMIT
        ),
    )(*fetched)


def unpack_kernel(
    early_hbm, late_hbm, state_hbm, embed_hbm,
    projection_out, kernel_out, gain_out, in_out, out_out, state_out, embed_out,
    early, late, state, embed, grad_projection, grad_kernel, grad_gain, grad_in, grad_out,
    load_sem, sems,
):
    loads = fetch(
        (early_hbm, late_hbm, state_hbm, embed_hbm), (early, late, state, embed), load_sem
    )
    channels, hidden = grad_in.shape
    features = grad_projection.shape[0]
    blocks = hidden // channels
    moves = [
        pltpu.make_async_copy(source, target, sems.at[number])
        for number, (source, target) in enumerate(
            (
                (state, state_out), (embed, embed_out), (grad_projection, projection_out),
                (grad_kernel, kernel_out), (grad_gain, gain_out), (grad_in, in_out),
                (grad_out, out_out),
            )
        )
    ]
    loads[0].wait()
    for k in range(blocks):
        columns = slice(k * channels, (k + 1) * channels)
        grad_in[:, columns] = early[pl.ds(k * channels, channels)].astype(jnp.float32)
    moves[5].start()
    loads[1].wait()
    grad_projection[...] = late[pl.ds(0, features)].astype(jnp.float32)
    moves[2].start()
    small = late[pl.ds(features, late.shape[0] - features)].astype(jnp.float32)
    for a in range(TAPS):
        grad_kernel[a] = small[a * TAPS : (a + 1) * TAPS]
    grad_gain[...] = small[TAPS * TAPS : TAPS * TAPS + 1]
    moves[3].start()
    moves[4].start()
    loads[2].wait()
    moves[0].start()
    loads[3].wait()
    moves[1].start()
    for k in range(blocks):
        columns = slice(k * channels, (k + 1) * channels)
        grad_out[columns, :] = jnp.transpose(
            early[pl.ds((blocks + k) * channels, channels)].astype(jnp.float32)
        )
    moves[6].start()
    for move in moves:
        move.wait()


def unpack(early, late, state, embed, channels, hidden, features):
    grads = (
        (features, channels), (TAPS, TAPS, channels), (1, channels),
        (channels, hidden), (hidden, channels),
    )
    shapes = grads + (state.shape, embed.shape)
    return pl.pallas_call(
        unpack_kernel,
        out_shape=tuple(jax.ShapeDtypeStruct(shape, jnp.float32) for shape in shapes),
        in_specs=[pl.BlockSpec(memory_space=pltpu.HBM)] * 4,
        out_specs=(pl.BlockSpec(memory_space=pltpu.HBM),) * 7,
        scratch_shapes=[VMEM(array.shape, array.dtype) for array in (early, late, state, embed)]
        + [VMEM(shape, jnp.float32) for shape in grads]
        + [pltpu.SemaphoreType.DMA((4,)), pltpu.SemaphoreType.DMA((7,))],
        compiler_params=pltpu.CompilerParams(vmem_limit_bytes=LIMIT),
    )(early, late, state, embed)


def shards(
    ocean_state,
    cotangent,
    atm_embed,
    projection,
    dw_kernel,
    norm_gain,
    w_in,
    w_out,
    margin_index,
    margin_weight,
    sea_mask,
):
    channels, hidden = w_in.shape
    state, embed, early, late = whole(
        jnp.transpose(margin_index, (1, 0, 2)), jnp.transpose(margin_weight, (1, 0, 2)),
        atm_embed, projection, ocean_state, dw_kernel, cotangent, sea_mask, norm_gain,
        w_in, w_out,
    )
    outs = unpack(early, late, state, embed, channels, hidden, atm_embed.shape[1])
    grad_projection, grad_kernel, grad_gain, grad_in, grad_out, grad_state, grad_embed = outs
    return (
        grad_state, grad_embed, grad_projection, grad_kernel,
        grad_gain.reshape(channels), grad_in, grad_out,
    )


def solution(mesh):
    return jax.shard_map(
        shards,
        mesh=mesh,
        in_specs=(
            P("lat", "lon", None),
            P("lat", "lon", None),
            P(("lat", "lon"), None),
            P(),
            P(),
            P(),
            P(),
            P(),
            P(None, "lat", "lon"),
            P(None, "lat", "lon"),
            P("lat", "lon"),
        ),
        out_specs=(P("lat", "lon", None), P(("lat", "lon"), None), P(), P(), P(), P(), P()),
        check_vma=False,
    )
```
